32 devices in a mesh: rows: 8 (over z, x), cols: 4 (over y, core).
Axes of the slice: x: 2, y: 2, z: 4, core: 2. Of those that a mesh axis runs over, the one named last changes fastest.
Arguments:
- source: float32 [1024, 32768], P('rows', 'cols'), may hold values from -6 to 6
- low_row: int32 [1024], replicated, may hold values from 0 to 1022, as said below
- weight_low: float32 [1024], replicated, may hold values from 0 to 1
Outputs:
- mercator: float32 [1024, 32768], P('rows', 'cols')
- level1: float32 [512, 16384], P('rows', 'cols')
- level2: float32 [256, 8192], P('rows', 'cols')
- level3: float32 [128, 4096], P(('rows', 'cols'))
- level4: float32 [64, 2048], P(('rows', 'cols'))
The draws below stay inside these ranges and needn't reach their ends.
Inputs may be any that keep to these rules, and one draw needn't show every extreme that they name: With t = 68 degrees in radians, E = ln tan(pi/4 + t/2), y = E * (1 - (2m + 1) / 2048) and lat = 2 atan(exp(y)) - pi/2, the base row of Mercator row m is floor((t - lat) / t * 1024 - 0.5) clipped to the range; low_row[m] differs from it by at most 2 and is then clipped to the range.
All inputs are finite; a program needn't handle non-finite values.
Results may differ from the reference program's by a relative error of at most 0.00007.
Values sent between devices are 32-bit elements; how exact they have to be, the bound alone decides.
A program may use at most 128 MiB of HBM per device.

```python
import math
import jax
import jax.numpy as jnp

TOTAL = 1024
COLS = 32768


def draw_low_row(key, part):
    window_top = 68.0 * math.pi / 180.0
    north_edge = math.log(math.tan(math.pi / 4 + window_top / 2))
    centres = (2.0 * jnp.arange(TOTAL, dtype=jnp.float32) + 1.0) / (2.0 * TOTAL)
    merc_y = north_edge * (1.0 - centres)
    latitude = 2.0 * jnp.arctan(jnp.exp(merc_y)) - math.pi / 2
    position = (window_top - latitude) / window_top * TOTAL - 0.5
    base_rows = jnp.clip(jnp.floor(position), 0, TOTAL - 2).astype(jnp.int32)
    jitter = jax.random.randint(key, (TOTAL,), -2, 3, dtype=jnp.int32)
    return jnp.clip(base_rows + jitter, 0, TOTAL - 2).astype(jnp.int32)


def shard_levels(rng, extent, shards, low, high):
    def one(axis_at, shards_of):
        draws = jax.random.uniform(jax.random.fold_in(jax.random.fold_in(rng, 6), axis_at), (shards_of,), jnp.float32, low / len(shards), high / len(shards))
        return jnp.repeat(jnp.exp(draws), extent[axis_at] // shards_of).reshape((-1,) + (1,) * (len(extent) - axis_at - 1))

    loudness = one(*shards[0])
    for cut in shards[1:]:
        loudness = loudness * one(*cut)
    return loudness


def normal_values(key, dims, width, reach, split=(), kind=jnp.bfloat16):
    entries = width * jax.random.normal(key, dims, jnp.float32)
    if split:
        entries = entries * shard_levels(key, dims, split, -0.22, 0.18)
    return jnp.clip(entries, -reach, reach).astype(kind)


def setup_inputs(seed: int = 0) -> dict:
    arg_keys = jax.random.split(jax.random.key(seed), 4)
    return {
        "source": normal_values(arg_keys[0], (TOTAL, COLS), 1.0, 6.0, ((0, 8), (1, 4)), jnp.float32),
        "low_row": draw_low_row(jax.random.fold_in(arg_keys[3], 71), 0),
        "weight_low": jnp.clip(jax.random.uniform(arg_keys[2], (TOTAL,), jnp.float32, 0.0, 1.0), 0.0, 1.0),
    }


def blend(columns, low_row, weight_low):
    upper_rows = jnp.take(columns, low_row, axis=0)
    lower_rows = jnp.take(columns, low_row + 1, axis=0)
    scales = weight_low.reshape((-1,) + (1,) * (columns.ndim - 1))
    return scales * upper_rows + (1.0 - scales) * lower_rows


def halve(picture):
    return (picture[0::2, 0::2] + picture[1::2, 0::2] + picture[0::2, 1::2] + picture[1::2, 1::2]) * 0.25


def reference(source, low_row, weight_low):
    mercator = blend(source, low_row, weight_low)
    level1 = halve(mercator)
    level2 = halve(level1)
    level3 = halve(level2)
    level4 = halve(level3)
    return (mercator, level1, level2, level3, level4)
```

```python
import functools
import math

import jax
import jax.numpy as jnp
import numpy as np
from jax import lax
from jax.experimental import pallas as pl
from jax.experimental.pallas import tpu as pltpu
from jax.sharding import PartitionSpec as P

LANES = 128
SUB = 8
WIDE = SUB * LANES
JITTER = 2
MESH = pl.DeviceIdType.MESH


def table(index, values):
    out = jnp.int32(values[0])
    for i in range(1, len(values)):
        if values[i] != values[i - 1]:
            out = jnp.where(index >= i, jnp.int32(values[i]), out)
    return out


@functools.lru_cache(maxsize=None)
def windows(total):
    top = 68.0 * math.pi / 180.0
    edge = math.log(math.tan(math.pi / 4 + top / 2))
    m = np.arange(total, dtype=np.float64)
    y = edge * (1.0 - (2.0 * m + 1.0) / (2.0 * total))
    lat = 2.0 * np.arctan(np.exp(y)) - math.pi / 2
    pos = (top - lat) / top * total - 0.5
    slack = 0.01 * total / 1024
    first = np.clip(np.clip(np.floor(pos - slack), 0, total - 2) - JITTER, 0, total - 2)
    last = np.clip(np.clip(np.floor(pos + slack), 0, total - 2) + JITTER, 0, total - 2) + 1
    return first.astype(int), last.astype(int)


@functools.lru_cache(maxsize=None)
def flows(total, parts):
    first, last = windows(total)
    block = total // parts
    found = {}
    for d in range(parts):
        mine = np.arange(d * block, (d + 1) * block)
        for s in range(parts):
            low, high = s * block, (s + 1) * block
            ms = mine[(last[mine] >= low) & (first[mine] < high)]
            if s == d or not len(ms):
                continue
            a, b = max(low, int(first[ms].min())), min(high - 1, int(last[ms].max()))
            m0, n = int(ms.min()), int(ms.max() - ms.min()) + 1
            found[s, d] = (False, a, b - a + 1) if b - a + 1 <= n else (True, m0, n)
    return found


def offsets(total, parts):
    send, recv, sent, got = {}, {}, [0] * parts, [0] * parts
    for (s, d), (_, _, n) in sorted(flows(total, parts).items()):
        send[s, d], recv[s, d] = sent[s], got[d]
        sent[s] += n
        got[d] += n
    return send, recv, sent, got


@functools.lru_cache(maxsize=None)
def relays(total, parts):
    moves = {k: n for k, (_, _, n) in flows(total, parts).items()}
    pairs = parts // 2
    if parts % 2 or min((d - s for s, d in moves), default=1) < 1 or max((d - s for s, d in moves), default=0) > 2:
        return {}
    plan, taken = {}, set()
    load = [moves.get((2 * z, 2 * z + 1), 0) for z in range(pairs)]
    across = 0.0
    for z in range(pairs - 1):
        across += load[z] - sum(load) / pairs
        n = int(round(abs(across)))
        at = z if across > 0 else z + 1
        key, relay = (2 * at, 2 * at + 1), 2 * at + (3 if across > 0 else -1)
        if n and n < moves.get(key, 0) and relay not in taken:
            plan.setdefault(key, {})[relay] = n
            taken.add(relay)
    back = [moves.get((2 * z + 1, 2 * z + 2), 0) for z in range(pairs - 1)]
    goal = sum(back) / pairs
    over = 0
    for z in range(pairs - 1):
        want = int(round(goal * (0.9 if z == 0 else 1.0))) - over
        n = max(0, min(want, back[z]))
        if n and 2 * z not in taken:
            plan.setdefault((2 * z + 1, 2 * z + 2), {})[2 * z] = n
            taken.add(2 * z)
            over = back[z] - n
        else:
            over = back[z]
    return plan


@functools.lru_cache(maxsize=None)
def legs(total, parts):
    send, recv, _, _ = offsets(total, parts)
    whole, out = {}, {}
    for (s, d), (_, _, n) in sorted(flows(total, parts).items()):
        at = 0
        for relay, rows in sorted(relays(total, parts).get((s, d), {}).items()):
            whole[relay - s, False, True, s] = (send[s, d] + at, 0, rows)
            whole[d - relay, True, False, relay] = (0, recv[s, d] + at, rows)
            at += rows
        if n > at:
            whole[d - s, False, False, s] = (send[s, d] + at, recv[s, d] + at, n - at)
    for (hop, relayed, relay, s), (at, to, n) in whole.items():
        done = 0
        for bit in reversed(range(n.bit_length())):
            if n >> bit & 1:
                out.setdefault((hop, relayed, relay, 1 << bit), {})[s] = (at + done, to + done)
                done += 1 << bit
    return sorted(out.items(), key=lambda item: item[0][:3] + (-item[0][3],))


def up(n, k):
    return -(-n // k) * k


def split(x):
    high = x.astype(jnp.bfloat16)
    low = (x - high.astype(jnp.float32)).astype(jnp.bfloat16)
    return high, low


def iota(shape, axis):
    return lax.broadcasted_iota(jnp.int32, shape, axis)


def pool_columns(x, levels):
    rows, width = x.shape
    slab = LANES << levels
    pairing = jnp.where(
        iota((slab, LANES), 0) >> levels == iota((slab, LANES), 1), 0.5**levels, 0.0
    ).astype(jnp.bfloat16)
    pieces = width // slab
    stacked = jnp.concatenate([x[:, k * slab : (k + 1) * slab] for k in range(pieces)], axis=0)
    high, low = split(stacked)
    out = jnp.dot(high, pairing, preferred_element_type=jnp.float32)
    out = out + jnp.dot(low, pairing, preferred_element_type=jnp.float32)
    return jnp.concatenate([out[k * rows : (k + 1) * rows] for k in range(pieces)], axis=1)


def exact_dot(a, b):
    return lax.dot_general(
        a,
        b,
        (((1,), (1,)), ((), ())),
        precision=lax.Precision.HIGHEST,
        preferred_element_type=jnp.float32,
    )


def flow_tables(total, parts, me, delta, kind, sending):
    send, recv, _, _ = offsets(total, parts)
    rows, place, first = [], [], []
    for i in range(parts):
        key = (i, i + delta) if sending else (i - delta, i)
        what = flows(total, parts).get(key)
        good = what is not None and what[0] == kind
        rows.append(what[2] if good else 0)
        place.append((send if sending else recv)[key] if good else 0)
        first.append(what[1] if good else 0)
    return table(me, rows), table(me, place), table(me, first)


def hops(total, parts, kind):
    return sorted({d - s for (s, d), what in flows(total, parts).items() if what[0] == kind})


def send_weights(total, parts, me, block, rows, low_ref, weight_ref):
    k, c = iota((rows, block), 0), iota((rows, block), 1)
    out = jnp.zeros((rows, block), jnp.float32)
    for delta in hops(total, parts, False):
        n, at, first = flow_tables(total, parts, me, delta, False, True)
        here = (k >= at) & (k < at + n)
        out = out + jnp.where(here & (c == k - at + first - me * block), 1.0, 0.0)
    for delta in hops(total, parts, True):
        n, at, first = flow_tables(total, parts, me, delta, True, True)
        owner = jnp.clip(me + delta, 0, parts - 1)
        low = low_ref[pl.ds(owner, 1), :] - me * block
        weight = weight_ref[pl.ds(owner, 1), :]
        row = iota((block, block), 0)
        band = jnp.where(row == low, weight, 0.0) + jnp.where(row == low + 1, 1.0 - weight, 0.0)
        pick = (k >= at) & (k < at + n) & (c == k - at + first - owner * block)
        out = out + exact_dot(jnp.where(pick, 1.0, 0.0), band)
    high, low_part = split(out)
    return jnp.concatenate([high, high, low_part], axis=1)


def own_weights(total, parts, me, block, slots, low_ref, weight_ref):
    low = low_ref[pl.ds(me, 1), :]
    weight = weight_ref[pl.ds(me, 1), :]

    def rows_of(g, valid):
        out = jnp.where(valid & (g == low), weight, 0.0)
        return out + jnp.where(valid & (g == low + 1), 1.0 - weight, 0.0)

    own = iota((block, block), 0) + me * block
    k, m = iota((slots, block), 0), iota((slots, block), 1)
    far = jnp.zeros((slots, block), jnp.float32)
    for delta in hops(total, parts, False):
        n, at, first = flow_tables(total, parts, me, delta, False, False)
        far = far + rows_of(k - at + first, (k >= at) & (k < at + n))
    for delta in hops(total, parts, True):
        n, at, first = flow_tables(total, parts, me, delta, True, False)
        here = (k >= at) & (k < at + n) & (m == k - at + first - me * block)
        far = far + jnp.where(here, 1.0, 0.0)
    band = jnp.concatenate([rows_of(own, own >= 0), far], axis=0)
    pools = []
    for level in range(4):
        o, i = iota((block >> level, block), 0), iota((block >> level, block), 1)
        pools.append(jnp.where(i >> level == o, 0.5**level, 0.0).astype(jnp.float32))
    high, low_part = split(exact_dot(jnp.concatenate(pools, axis=0), band))
    return jnp.concatenate([high, high, low_part], axis=1)


def fused_kernel(
    total, parts, owners,
    low_ref, weight_ref, source_ref,
    merc_ref, one_ref, two_ref, rows_ref, pooled_ref,
    own, sent, recv, held, three, landed, out_w, in_w,
    own_sem, send_sem, recv_sem, share_send, share_recv,
):
    block, width = source_ref.shape
    chunks = width // WIDE
    me, col = lax.axis_index("rows"), lax.axis_index("cols")
    groups = legs(total, parts)
    got = table(me, offsets(total, parts)[3])
    slots = recv.shape[1]
    send_rows = sent.shape[1]

    def columns(j, size):
        return pl.ds(pl.multiple_of(j * size, size), size)

    def load(j):
        at = columns(j, WIDE)
        return pltpu.make_async_copy(source_ref.at[:, at], own.at[:, at], own_sem.at[j])

    @pl.loop(0, chunks)
    def _(j):
        load(j).start()

    barrier = pltpu.get_barrier_semaphore()
    greet = {}
    for (hop, _, _, _), by in groups:
        for s in by:
            greet.setdefault(hop, set()).add(s)
            greet.setdefault(-hop, set()).add(s + hop)
    for hop, who in sorted(greet.items()):
        @pl.when(table(me, [int(i in who) for i in range(parts)]) > 0)
        def _():
            pl.semaphore_signal(barrier, inc=1, device_id={"rows": me + hop}, device_id_type=MESH)

    for i in range(1, owners):
        pl.semaphore_signal(
            barrier, inc=1, device_id={"cols": lax.rem(col + i, owners)}, device_id_type=MESH
        )
    waits = [sum(i in who for who in greet.values()) + owners - 1 for i in range(parts)]

    def copy(g, j, src, dst, target):
        return pltpu.make_async_remote_copy(
            src_ref=src,
            dst_ref=dst,
            send_sem=send_sem.at[g, j],
            recv_sem=recv_sem.at[g, j],
            device_id={"rows": target},
            device_id_type=MESH,
        )

    def leaving(g, j, act):
        (hop, relayed, to_relay, n), by = groups[g]
        at, to = (table(me, [by.get(i, (0, 0))[f] for i in range(parts)]) for f in range(2))
        src, dst = (held if relayed else sent), (held if to_relay else recv)

        @pl.when(table(me, [int(i in by) for i in range(parts)]) > 0)
        def _():
            act(copy(g, j, src.at[j, pl.ds(at, n)], dst.at[j, pl.ds(to, n)], me + hop))

    def arriving(g, j):
        (hop, _, to_relay, n), by = groups[g]
        to = table(me, [by.get(i - hop, (0, 0))[1] for i in range(parts)])
        dst = held if to_relay else recv

        @pl.when(table(me, [int(i - hop in by) for i in range(parts)]) > 0)
        def _():
            there = dst.at[j, pl.ds(to, n)]
            copy(g, j, there, there, me - hop).wait_recv()

    first_hop = [g for g, ((_, relayed, _, _), _) in enumerate(groups) if not relayed]
    second_hop = [g for g, ((_, relayed, _, _), _) in enumerate(groups) if relayed]
    to_relay = [g for g, ((_, _, relay, _), _) in enumerate(groups) if relay]
    to_owner = [g for g, ((_, _, relay, _), _) in enumerate(groups) if not relay]
    first_hop.sort(key=lambda g: g not in to_relay)

    out_w[...] = send_weights(total, parts, me, block, send_rows, low_ref, weight_ref)
    sent_rows = sent.reshape(chunks, send_rows * SUB, LANES)
    recv_rows = recv.reshape(chunks, slots * SUB, LANES)

    def prepare(j):
        load(j).wait()
        high, low_part = split(own[:, columns(j, WIDE)])
        y = jnp.dot(
            out_w[...],
            jnp.concatenate([high, low_part, high], axis=0),
            preferred_element_type=jnp.float32,
        )
        for b in range(SUB):
            sent_rows[j, pl.ds(b, send_rows, stride=SUB), :] = y[:, b * LANES : (b + 1) * LANES]

    def dispatch(j):
        for g in first_hop:
            leaving(g, j, lambda c: c.start())

    prepare(0)
    pl.semaphore_wait(barrier, table(me, waits))
    dispatch(0)

    @pl.loop(1, chunks)
    def _(j):
        prepare(j)
        dispatch(j)

    in_w[...] = own_weights(total, parts, me, block, slots, low_ref, weight_ref)

    def forward(j):
        for g in to_relay:
            arriving(g, j)
        for g in second_hop:
            leaving(g, j, lambda c: c.start())

    forward(0)

    @pl.loop(0, chunks)
    def _(j):
        @pl.when(j + 1 < chunks)
        def _():
            forward(j + 1)

        for g in to_owner:
            arriving(g, j)
        row = iota((slots, LANES), 0)
        far = [
            jnp.where(row < got, recv_rows[j, pl.ds(b, slots, stride=SUB), :], 0.0)
            for b in range(SUB)
        ]
        x = jnp.concatenate([own[:, columns(j, WIDE)], jnp.concatenate(far, axis=1)], axis=0)
        high, low_part = split(x)
        y = jnp.dot(
            in_w[...],
            jnp.concatenate([high, low_part, high], axis=0),
            preferred_element_type=jnp.float32,
        )
        merc_ref[:, columns(j, WIDE)] = y[:block]
        at = block
        for level, ref in ((1, one_ref), (2, two_ref)):
            n = block >> level
            ref[:, columns(j, WIDE >> level)] = pool_columns(y[at : at + n], level)
            at += n
        pooled = pool_columns(y[at:], 3)
        each = three.shape[1]
        for i in range(owners):
            three[i, :, columns(j, WIDE >> 3)] = pooled[i * each : (i + 1) * each]

    shares = []
    for i in range(1, owners):
        target = lax.rem(col + i, owners)
        shares.append(
            pltpu.make_async_remote_copy(
                src_ref=three.at[target],
                dst_ref=landed.at[owners - i],
                send_sem=share_send.at[i],
                recv_sem=share_recv.at[owners - i],
                device_id={"cols": target},
                device_id_type=MESH,
            )
        )
    for c in shares:
        c.start()

    @pl.loop(0, chunks)
    def _(j):
        for g in range(len(groups)):
            leaving(g, j, lambda c: c.wait_send())

    landed[0] = three[col]
    for c in shares:
        c.wait()
    finish(owners, col, landed, rows_ref, pooled_ref)


def finish(owners, col, landed, rows_ref, pooled_ref):
    _, each, width = landed.shape
    pairs = each // 2
    slab = 2 * LANES
    pairing = jnp.where(
        iota((slab, LANES), 0) >> 1 == iota((slab, LANES), 1), 0.25, 0.0
    ).astype(jnp.bfloat16)
    x = jnp.concatenate([landed[lax.rem(c - col + owners, owners)] for c in range(owners)], axis=1)
    rows_ref[...] = x
    sums = jnp.concatenate(
        [x[2 * p : 2 * p + 1] + x[2 * p + 1 : 2 * p + 2] for p in range(pairs)], axis=0
    )
    count = owners * width // slab
    flat = jnp.concatenate([sums[:, k * slab : (k + 1) * slab] for k in range(count)], axis=0)
    high, low_part = split(flat)
    out = jnp.dot(high, pairing, preferred_element_type=jnp.float32)
    out = out + jnp.dot(low_part, pairing, preferred_element_type=jnp.float32)
    pooled_ref[...] = jnp.concatenate(
        [out[k * pairs : (k + 1) * pairs] for k in range(count)], axis=1
    )


def write_kernel(*refs):
    n = len(refs) // 2
    sems = refs[2 * n]
    copies = [pltpu.make_async_copy(refs[i], refs[n + i], sems.at[i]) for i in range(n)]
    for c in copies:
        c.start()
    for c in copies:
        c.wait()


def body(parts, owners, source, low_row, weight_low):
    total = low_row.shape[0]
    block, width = source.shape
    _, _, sent, got = offsets(total, parts)
    send_rows, slots = up(max(sent), 16), up(max(got), 16)
    hold = max([n for by in relays(total, parts).values() for n in by.values()], default=1)
    groups = max(len(legs(total, parts)), 1)
    chunks = width // WIDE
    each = (block >> 3) // owners
    wide_rows = block + block // 2 + block // 4 + block // 8
    f32 = jnp.float32
    shapes = [(block >> k, width >> k) for k in range(3)]
    shapes += [(each, owners * (width >> 3)), (each // 2, owners * (width >> 4))]
    vmem = pl.BlockSpec(memory_space=pltpu.VMEM)
    hbm = pl.BlockSpec(memory_space=pltpu.HBM)
    outs = pl.pallas_call(
        functools.partial(fused_kernel, total, parts, owners),
        out_shape=[pltpu.VMEM(s, f32) for s in shapes],
        in_specs=[vmem, vmem, hbm],
        out_specs=[vmem] * len(shapes),
        scratch_shapes=[
            pltpu.VMEM((block, width), f32),
            pltpu.VMEM((chunks, send_rows, SUB, LANES), f32),
            pltpu.VMEM((chunks, slots, SUB, LANES), f32),
            pltpu.VMEM((chunks, hold, SUB, LANES), f32),
            pltpu.VMEM((owners, each, width >> 3), f32),
            pltpu.VMEM((owners, each, width >> 3), f32),
            pltpu.VMEM((send_rows, 3 * block), jnp.bfloat16),
            pltpu.VMEM((wide_rows, 3 * (block + slots)), jnp.bfloat16),
            pltpu.SemaphoreType.DMA((chunks,)),
            pltpu.SemaphoreType.DMA((groups, chunks)),
            pltpu.SemaphoreType.DMA((groups, chunks)),
            pltpu.SemaphoreType.DMA((owners,)),
            pltpu.SemaphoreType.DMA((owners,)),
        ],
        compiler_params=pltpu.CompilerParams(
            collective_id=0, has_side_effects=True, vmem_limit_bytes=54 << 20
        ),
        name="reproject",
    )(low_row.reshape(parts, block), weight_low.reshape(parts, block), source)
    return pl.pallas_call(
        write_kernel,
        out_shape=[jax.ShapeDtypeStruct(s, f32) for s in shapes],
        in_specs=[vmem] * len(shapes),
        out_specs=[hbm] * len(shapes),
        scratch_shapes=[pltpu.SemaphoreType.DMA((len(shapes),))],
        compiler_params=pltpu.CompilerParams(vmem_limit_bytes=8 << 20),
        name="write",
    )(*outs)


def solution(mesh):
    return jax.shard_map(
        functools.partial(body, mesh.shape["rows"], mesh.shape["cols"]),
        mesh=mesh,
        in_specs=(P("rows", "cols"), P(), P()),
        out_specs=(
            P("rows", "cols"),
            P("rows", "cols"),
            P("rows", "cols"),
            P(("rows", "cols"), None),
            P(("rows", "cols"), None),
        ),
        check_vma=False,
    )
```

```python
import functools
import math

import jax
import jax.numpy as jnp
import numpy as np
from jax import lax
from jax.experimental import pallas as pl
from jax.experimental.pallas import tpu as pltpu
from jax.sharding import PartitionSpec as P

LANES = 128
SUB = 8
WIDE = SUB * LANES
JITTER = 2
MESH = pl.DeviceIdType.MESH


def table(index, values):
    out = jnp.int32(values[0])
    for i in range(1, len(values)):
        if values[i] != values[i - 1]:
            out = jnp.where(index >= i, jnp.int32(values[i]), out)
    return out


@functools.lru_cache(maxsize=None)
def windows(total):
    top = 68.0 * math.pi / 180.0
    edge = math.log(math.tan(math.pi / 4 + top / 2))
    m = np.arange(total, dtype=np.float64)
    y = edge * (1.0 - (2.0 * m + 1.0) / (2.0 * total))
    lat = 2.0 * np.arctan(np.exp(y)) - math.pi / 2
    pos = (top - lat) / top * total - 0.5
    slack = 0.01 * total / 1024
    first = np.clip(np.clip(np.floor(pos - slack), 0, total - 2) - JITTER, 0, total - 2)
    last = np.clip(np.clip(np.floor(pos + slack), 0, total - 2) + JITTER, 0, total - 2) + 1
    return first.astype(int), last.astype(int)


@functools.lru_cache(maxsize=None)
def flows(total, parts):
    first, last = windows(total)
    block = total // parts
    found = {}
    for d in range(parts):
        mine = np.arange(d * block, (d + 1) * block)
        for s in range(parts):
            low, high = s * block, (s + 1) * block
            ms = mine[(last[mine] >= low) & (first[mine] < high)]
            if s == d or not len(ms):
                continue
            a, b = max(low, int(first[ms].min())), min(high - 1, int(last[ms].max()))
            m0, n = int(ms.min()), int(ms.max() - ms.min()) + 1
            found[s, d] = (False, a, b - a + 1) if b - a + 1 <= n else (True, m0, n)
    return found


def offsets(total, parts):
    send, recv, sent, got = {}, {}, [0] * parts, [0] * parts
    for (s, d), (_, _, n) in sorted(flows(total, parts).items()):
        send[s, d], recv[s, d] = sent[s], got[d]
        sent[s] += n
        got[d] += n
    return send, recv, sent, got


@functools.lru_cache(maxsize=None)
def relays(total, parts):
    moves = {k: n for k, (_, _, n) in flows(total, parts).items()}
    pairs = parts // 2
    if parts % 2 or min((d - s for s, d in moves), default=1) < 1 or max((d - s for s, d in moves), default=0) > 2:
        return {}
    plan, taken = {}, set()
    load = [moves.get((2 * z, 2 * z + 1), 0) for z in range(pairs)]
    across = 0.0
    for z in range(pairs - 1):
        across += load[z] - sum(load) / pairs
        n = int(round(abs(across)))
        at = z if across > 0 else z + 1
        key, relay = (2 * at, 2 * at + 1), 2 * at + (3 if across > 0 else -1)
        if n and n < moves.get(key, 0) and relay not in taken:
            plan.setdefault(key, {})[relay] = n
            taken.add(relay)
    back = [moves.get((2 * z + 1, 2 * z + 2), 0) for z in range(pairs - 1)]
    goal = sum(back) / pairs
    over = 0
    for z in range(pairs - 1):
        want = int(round(goal * (0.9 if z == 0 else 1.0))) - over
        n = max(0, min(want, back[z]))
        if n and 2 * z not in taken:
            plan.setdefault((2 * z + 1, 2 * z + 2), {})[2 * z] = n
            taken.add(2 * z)
            over = back[z] - n
        else:
            over = back[z]
    return plan


@functools.lru_cache(maxsize=None)
def legs(total, parts):
    send, recv, _, _ = offsets(total, parts)
    found = []
    for (s, d), (_, _, n) in sorted(flows(total, parts).items()):
        at = 0
        for relay, rows in sorted(relays(total, parts).get((s, d), {}).items()):
            found.append((s, relay, False, True, send[s, d] + at, 0, rows))
            found.append((relay, d, True, False, 0, recv[s, d] + at, rows))
            at += rows
        if n > at:
            found.append((s, d, False, False, send[s, d] + at, recv[s, d] + at, n - at))
    found.sort(key=lambda leg: not leg[3])
    left, come, out = [0] * parts, [0] * parts, []
    for leg in found:
        out.append(leg + (left[leg[0]], come[leg[1]]))
        left[leg[0]] += 1
        come[leg[1]] += 1
    return out


def up(n, k):
    return -(-n // k) * k


def split(x):
    high = x.astype(jnp.bfloat16)
    low = (x - high.astype(jnp.float32)).astype(jnp.bfloat16)
    return high, low


def iota(shape, axis):
    return lax.broadcasted_iota(jnp.int32, shape, axis)


def pool_columns(x, levels):
    rows, width = x.shape
    slab = LANES << levels
    pairing = jnp.where(
        iota((slab, LANES), 0) >> levels == iota((slab, LANES), 1), 0.5**levels, 0.0
    ).astype(jnp.bfloat16)
    pieces = width // slab
    stacked = jnp.concatenate([x[:, k * slab : (k + 1) * slab] for k in range(pieces)], axis=0)
    high, low = split(stacked)
    out = jnp.dot(high, pairing, preferred_element_type=jnp.float32)
    out = out + jnp.dot(low, pairing, preferred_element_type=jnp.float32)
    return jnp.concatenate([out[k * rows : (k + 1) * rows] for k in range(pieces)], axis=1)


def exact_dot(a, b):
    return lax.dot_general(
        a,
        b,
        (((1,), (1,)), ((), ())),
        precision=lax.Precision.HIGHEST,
        preferred_element_type=jnp.float32,
    )


def flow_tables(total, parts, me, delta, kind, sending):
    send, recv, _, _ = offsets(total, parts)
    rows, place, first = [], [], []
    for i in range(parts):
        key = (i, i + delta) if sending else (i - delta, i)
        what = flows(total, parts).get(key)
        good = what is not None and what[0] == kind
        rows.append(what[2] if good else 0)
        place.append((send if sending else recv)[key] if good else 0)
        first.append(what[1] if good else 0)
    return table(me, rows), table(me, place), table(me, first)


def hops(total, parts, kind):
    return sorted({d - s for (s, d), what in flows(total, parts).items() if what[0] == kind})


def send_weights(total, parts, me, block, rows, low_ref, weight_ref):
    k, c = iota((rows, block), 0), iota((rows, block), 1)
    out = jnp.zeros((rows, block), jnp.float32)
    for delta in hops(total, parts, False):
        n, at, first = flow_tables(total, parts, me, delta, False, True)
        here = (k >= at) & (k < at + n)
        out = out + jnp.where(here & (c == k - at + first - me * block), 1.0, 0.0)
    for delta in hops(total, parts, True):
        n, at, first = flow_tables(total, parts, me, delta, True, True)
        owner = jnp.clip(me + delta, 0, parts - 1)
        low = low_ref[pl.ds(owner, 1), :] - me * block
        weight = weight_ref[pl.ds(owner, 1), :]
        row = iota((block, block), 0)
        band = jnp.where(row == low, weight, 0.0) + jnp.where(row == low + 1, 1.0 - weight, 0.0)
        pick = (k >= at) & (k < at + n) & (c == k - at + first - owner * block)
        out = out + exact_dot(jnp.where(pick, 1.0, 0.0), band)
    high, low_part = split(out)
    return jnp.concatenate([high, high, low_part], axis=1)


def own_weights(total, parts, me, block, slots, low_ref, weight_ref):
    low = low_ref[pl.ds(me, 1), :]
    weight = weight_ref[pl.ds(me, 1), :]

    def rows_of(g, valid):
        out = jnp.where(valid & (g == low), weight, 0.0)
        return out + jnp.where(valid & (g == low + 1), 1.0 - weight, 0.0)

    own = iota((block, block), 0) + me * block
    k, m = iota((slots, block), 0), iota((slots, block), 1)
    far = jnp.zeros((slots, block), jnp.float32)
    for delta in hops(total, parts, False):
        n, at, first = flow_tables(total, parts, me, delta, False, False)
        far = far + rows_of(k - at + first, (k >= at) & (k < at + n))
    for delta in hops(total, parts, True):
        n, at, first = flow_tables(total, parts, me, delta, True, False)
        here = (k >= at) & (k < at + n) & (m == k - at + first - me * block)
        far = far + jnp.where(here, 1.0, 0.0)
    band = jnp.concatenate([rows_of(own, own >= 0), far], axis=0)
    pools = []
    for level in range(4):
        o, i = iota((block >> level, block), 0), iota((block >> level, block), 1)
        pools.append(jnp.where(i >> level == o, 0.5**level, 0.0).astype(jnp.float32))
    high, low_part = split(exact_dot(jnp.concatenate(pools, axis=0), band))
    return jnp.concatenate([high, high, low_part], axis=1)


def fused_kernel(
    total, parts, owners,
    low_ref, weight_ref, source_ref,
    merc_ref, one_ref, two_ref, rows_ref, pooled_ref,
    own, sent, recv, held, three, landed, out_w, in_w,
    own_sem, send_sem, recv_sem, share_send, share_recv,
):
    block, width = source_ref.shape
    chunks = width // WIDE
    me, col = lax.axis_index("rows"), lax.axis_index("cols")
    groups = legs(total, parts)
    got = table(me, offsets(total, parts)[3])
    slots = recv.shape[1]
    send_rows = sent.shape[1]

    def columns(j, size):
        return pl.ds(pl.multiple_of(j * size, size), size)

    def load(j):
        at = columns(j, WIDE)
        return pltpu.make_async_copy(source_ref.at[:, at], own.at[:, at], own_sem.at[j])

    @pl.loop(0, chunks)
    def _(j):
        load(j).start()

    def by_device(chosen, act, where):
        for i in range(parts):
            mine = [leg for leg in chosen if leg[where] == i]

            if mine:
                @pl.when(me == i)
                def _():
                    for leg in mine:
                        act(leg)

    barrier = pltpu.get_barrier_semaphore()
    met = [sorted({a[1 - k] for a in groups for k in (0, 1) if a[k] == i}) for i in range(parts)]
    for i in range(parts):
        @pl.when(me == i)
        def _():
            for other in met[i]:
                pl.semaphore_signal(barrier, inc=1, device_id={"rows": other}, device_id_type=MESH)

    for i in range(1, owners):
        pl.semaphore_signal(
            barrier, inc=1, device_id={"cols": lax.rem(col + i, owners)}, device_id_type=MESH
        )
    waits = [len(met[i]) + owners - 1 for i in range(parts)]

    def copy(leg, j):
        _, target, relayed, to_relay, at, to, n, left, come = leg
        src, dst = (held if relayed else sent), (held if to_relay else recv)
        return pltpu.make_async_remote_copy(
            src_ref=src.at[j, pl.ds(at, n)],
            dst_ref=dst.at[j, pl.ds(to, n)],
            send_sem=send_sem.at[left, j],
            recv_sem=recv_sem.at[come, j],
            device_id={"rows": target},
            device_id_type=MESH,
        )

    def leave(chosen, j):
        by_device(chosen, lambda leg: copy(leg, j).start(), 0)

    def arrive(chosen, j):
        by_device(chosen, lambda leg: copy(leg, j).wait_recv(), 1)

    first_hop = [leg for leg in groups if not leg[2]]
    second_hop = [leg for leg in groups if leg[2]]
    to_relay = [leg for leg in groups if leg[3]]
    to_owner = [leg for leg in groups if not leg[3]]

    out_w[...] = send_weights(total, parts, me, block, send_rows, low_ref, weight_ref)
    sent_rows = sent.reshape(chunks, send_rows * SUB, LANES)
    recv_rows = recv.reshape(chunks, slots * SUB, LANES)

    def prepare(j):
        load(j).wait()
        high, low_part = split(own[:, columns(j, WIDE)])
        y = jnp.dot(
            out_w[...],
            jnp.concatenate([high, low_part, high], axis=0),
            preferred_element_type=jnp.float32,
        )
        for b in range(SUB):
            sent_rows[j, pl.ds(b, send_rows, stride=SUB), :] = y[:, b * LANES : (b + 1) * LANES]

    prepare(0)
    pl.semaphore_wait(barrier, table(me, waits))
    leave(first_hop, 0)

    @pl.loop(1, chunks)
    def _(j):
        prepare(j)
        leave(first_hop, j)

    in_w[...] = own_weights(total, parts, me, block, slots, low_ref, weight_ref)

    def forward(j):
        arrive(to_relay, j)
        leave(second_hop, j)

    forward(0)

    @pl.loop(0, chunks)
    def _(j):
        @pl.when(j + 1 < chunks)
        def _():
            forward(j + 1)

        arrive(to_owner, j)
        row = iota((slots, LANES), 0)
        far = [
            jnp.where(row < got, recv_rows[j, pl.ds(b, slots, stride=SUB), :], 0.0)
            for b in range(SUB)
        ]
        x = jnp.concatenate([own[:, columns(j, WIDE)], jnp.concatenate(far, axis=1)], axis=0)
        high, low_part = split(x)
        y = jnp.dot(
            in_w[...],
            jnp.concatenate([high, low_part, high], axis=0),
            preferred_element_type=jnp.float32,
        )
        merc_ref[:, columns(j, WIDE)] = y[:block]
        at = block
        for level, ref in ((1, one_ref), (2, two_ref)):
            n = block >> level
            ref[:, columns(j, WIDE >> level)] = pool_columns(y[at : at + n], level)
            at += n
        pooled = pool_columns(y[at:], 3)
        each = three.shape[1]
        for i in range(owners):
            three[i, :, columns(j, WIDE >> 3)] = pooled[i * each : (i + 1) * each]

    shares = []
    for i in range(1, owners):
        target = lax.rem(col + i, owners)
        shares.append(
            pltpu.make_async_remote_copy(
                src_ref=three.at[target],
                dst_ref=landed.at[owners - i],
                send_sem=share_send.at[i],
                recv_sem=share_recv.at[owners - i],
                device_id={"cols": target},
                device_id_type=MESH,
            )
        )
    for c in shares:
        c.start()

    @pl.loop(0, chunks)
    def _(j):
        by_device(groups, lambda leg: copy(leg, j).wait_send(), 0)

    landed[0] = three[col]
    for c in shares:
        c.wait()
    finish(owners, col, landed, rows_ref, pooled_ref)


def finish(owners, col, landed, rows_ref, pooled_ref):
    _, each, width = landed.shape
    pairs = each // 2
    slab = 2 * LANES
    pairing = jnp.where(
        iota((slab, LANES), 0) >> 1 == iota((slab, LANES), 1), 0.25, 0.0
    ).astype(jnp.bfloat16)
    x = jnp.concatenate([landed[lax.rem(c - col + owners, owners)] for c in range(owners)], axis=1)
    rows_ref[...] = x
    sums = jnp.concatenate(
        [x[2 * p : 2 * p + 1] + x[2 * p + 1 : 2 * p + 2] for p in range(pairs)], axis=0
    )
    count = owners * width // slab
    flat = jnp.concatenate([sums[:, k * slab : (k + 1) * slab] for k in range(count)], axis=0)
    high, low_part = split(flat)
    out = jnp.dot(high, pairing, preferred_element_type=jnp.float32)
    out = out + jnp.dot(low_part, pairing, preferred_element_type=jnp.float32)
    pooled_ref[...] = jnp.concatenate(
        [out[k * pairs : (k + 1) * pairs] for k in range(count)], axis=1
    )


def write_kernel(*refs):
    n = len(refs) // 2
    sems = refs[2 * n]
    copies = [pltpu.make_async_copy(refs[i], refs[n + i], sems.at[i]) for i in range(n)]
    for c in copies:
        c.start()
    for c in copies:
        c.wait()


def body(parts, owners, source, low_row, weight_low):
    total = low_row.shape[0]
    block, width = source.shape
    _, _, sent, got = offsets(total, parts)
    send_rows, slots = up(max(sent), 16), up(max(got), 16)
    hold = max([n for by in relays(total, parts).values() for n in by.values()], default=1)
    left = max([leg[7] + 1 for leg in legs(total, parts)], default=1)
    come = max([leg[8] + 1 for leg in legs(total, parts)], default=1)
    chunks = width // WIDE
    each = (block >> 3) // owners
    wide_rows = block + block // 2 + block // 4 + block // 8
    f32 = jnp.float32
    shapes = [(block >> k, width >> k) for k in range(3)]
    shapes += [(each, owners * (width >> 3)), (each // 2, owners * (width >> 4))]
    vmem = pl.BlockSpec(memory_space=pltpu.VMEM)
    hbm = pl.BlockSpec(memory_space=pltpu.HBM)
    outs = pl.pallas_call(
        functools.partial(fused_kernel, total, parts, owners),
        out_shape=[pltpu.VMEM(s, f32) for s in shapes],
        in_specs=[vmem, vmem, hbm],
        out_specs=[vmem] * len(shapes),
        scratch_shapes=[
            pltpu.VMEM((block, width), f32),
            pltpu.VMEM((chunks, send_rows, SUB, LANES), f32),
            pltpu.VMEM((chunks, slots, SUB, LANES), f32),
            pltpu.VMEM((chunks, hold, SUB, LANES), f32),
            pltpu.VMEM((owners, each, width >> 3), f32),
            pltpu.VMEM((owners, each, width >> 3), f32),
            pltpu.VMEM((send_rows, 3 * block), jnp.bfloat16),
            pltpu.VMEM((wide_rows, 3 * (block + slots)), jnp.bfloat16),
            pltpu.SemaphoreType.DMA((chunks,)),
            pltpu.SemaphoreType.DMA((left, chunks)),
            pltpu.SemaphoreType.DMA((come, chunks)),
            pltpu.SemaphoreType.DMA((owners,)),
            pltpu.SemaphoreType.DMA((owners,)),
        ],
        compiler_params=pltpu.CompilerParams(
            collective_id=0, has_side_effects=True, vmem_limit_bytes=54 << 20
        ),
        name="reproject",
    )(low_row.reshape(parts, block), weight_low.reshape(parts, block), source)
    return pl.pallas_call(
        write_kernel,
        out_shape=[jax.ShapeDtypeStruct(s, f32) for s in shapes],
        in_specs=[vmem] * len(shapes),
        out_specs=[hbm] * len(shapes),
        scratch_shapes=[pltpu.SemaphoreType.DMA((len(shapes),))],
        compiler_params=pltpu.CompilerParams(vmem_limit_bytes=8 << 20),
        name="write",
    )(*outs)


def solution(mesh):
    return jax.shard_map(
        functools.partial(body, mesh.shape["rows"], mesh.shape["cols"]),
        mesh=mesh,
        in_specs=(P("rows", "cols"), P(), P()),
        out_specs=(
            P("rows", "cols"),
            P("rows", "cols"),
            P("rows", "cols"),
            P(("rows", "cols"), None),
            P(("rows", "cols"), None),
        ),
        check_vma=False,
    )
```

```python
import functools
import math

import jax
import jax.numpy as jnp
import numpy as np
from jax import lax
from jax.experimental import pallas as pl
from jax.experimental.pallas import tpu as pltpu
from jax.sharding import PartitionSpec as P

LANES = 128
SUB = 8
WIDE = SUB * LANES
JITTER = 2
HINTED = 2
MESH = pl.DeviceIdType.MESH


def table(index, values):
    out = jnp.int32(values[0])
    for i in range(1, len(values)):
        if values[i] != values[i - 1]:
            out = jnp.where(index >= i, jnp.int32(values[i]), out)
    return out


@functools.lru_cache(maxsize=None)
def windows(total):
    top = 68.0 * math.pi / 180.0
    edge = math.log(math.tan(math.pi / 4 + top / 2))
    m = np.arange(total, dtype=np.float64)
    y = edge * (1.0 - (2.0 * m + 1.0) / (2.0 * total))
    lat = 2.0 * np.arctan(np.exp(y)) - math.pi / 2
    pos = (top - lat) / top * total - 0.5
    slack = 0.01 * total / 1024
    first = np.clip(np.clip(np.floor(pos - slack), 0, total - 2) - JITTER, 0, total - 2)
    last = np.clip(np.clip(np.floor(pos + slack), 0, total - 2) + JITTER, 0, total - 2) + 1
    return first.astype(int), last.astype(int)


@functools.lru_cache(maxsize=None)
def flows(total, parts):
    first, last = windows(total)
    block = total // parts
    found = {}
    for d in range(parts):
        mine = np.arange(d * block, (d + 1) * block)
        for s in range(parts):
            low, high = s * block, (s + 1) * block
            ms = mine[(last[mine] >= low) & (first[mine] < high)]
            if s == d or not len(ms):
                continue
            a, b = max(low, int(first[ms].min())), min(high - 1, int(last[ms].max()))
            m0, n = int(ms.min()), int(ms.max() - ms.min()) + 1
            found[s, d] = (False, a, b - a + 1) if b - a + 1 <= n else (True, m0, n)
    return found


def offsets(total, parts):
    send, recv, sent, got = {}, {}, [0] * parts, [0] * parts
    for (s, d), (_, _, n) in sorted(flows(total, parts).items()):
        send[s, d], recv[s, d] = sent[s], got[d]
        sent[s] += n
        got[d] += n
    return send, recv, sent, got


@functools.lru_cache(maxsize=None)
def relays(total, parts):
    moves = {k: n for k, (_, _, n) in flows(total, parts).items()}
    pairs = parts // 2
    if parts % 2 or min((d - s for s, d in moves), default=1) < 1 or max((d - s for s, d in moves), default=0) > 2:
        return {}
    plan, taken = {}, set()
    load = [moves.get((2 * z, 2 * z + 1), 0) for z in range(pairs)]
    across = 0.0
    for z in range(pairs - 1):
        across += load[z] - sum(load) / pairs
        n = int(round(abs(across)))
        at = z if across > 0 else z + 1
        key, relay = (2 * at, 2 * at + 1), 2 * at + (3 if across > 0 else -1)
        if n and n < moves.get(key, 0) and relay not in taken:
            plan.setdefault(key, {})[relay] = n
            taken.add(relay)
    back = [moves.get((2 * z + 1, 2 * z + 2), 0) for z in range(pairs - 1)]
    goal = sum(back) / pairs
    over = 0
    for z in range(pairs - 1):
        want = int(round(goal * (0.9 if z == 0 else 1.0))) - over
        n = max(0, min(want, back[z]))
        if n and 2 * z not in taken:
            plan.setdefault((2 * z + 1, 2 * z + 2), {})[2 * z] = n
            taken.add(2 * z)
            over = back[z] - n
        else:
            over = back[z]
    return plan


def halves(n):
    return [(0, n // 2), (n // 2, n - n // 2)] if n > 1 else [(0, n)]


@functools.lru_cache(maxsize=None)
def legs(total, parts):
    send, recv, _, _ = offsets(total, parts)
    found = []
    for (s, d), (_, _, n) in sorted(flows(total, parts).items()):
        at = 0
        for relay, rows in sorted(relays(total, parts).get((s, d), {}).items()):
            for half, (low, n_part) in enumerate(halves(rows)):
                found.append((s, relay, False, True, send[s, d] + at + low, low, n_part, half))
                found.append((relay, d, True, False, low, recv[s, d] + at + low, n_part, half))
            at += rows
        if n > at:
            found.append((s, d, False, False, send[s, d] + at, recv[s, d] + at, n - at, 0))
    return sorted(found, key=lambda leg: not leg[3])


def up(n, k):
    return -(-n // k) * k


def split(x):
    high = x.astype(jnp.bfloat16)
    low = (x - high.astype(jnp.float32)).astype(jnp.bfloat16)
    return high, low


def iota(shape, axis):
    return lax.broadcasted_iota(jnp.int32, shape, axis)


def pool_columns(x, levels):
    rows, width = x.shape
    slab = LANES << levels
    pairing = jnp.where(
        iota((slab, LANES), 0) >> levels == iota((slab, LANES), 1), 0.5**levels, 0.0
    ).astype(jnp.bfloat16)
    pieces = width // slab
    stacked = jnp.concatenate([x[:, k * slab : (k + 1) * slab] for k in range(pieces)], axis=0)
    high, low = split(stacked)
    out = jnp.dot(high, pairing, preferred_element_type=jnp.float32)
    out = out + jnp.dot(low, pairing, preferred_element_type=jnp.float32)
    return jnp.concatenate([out[k * rows : (k + 1) * rows] for k in range(pieces)], axis=1)


def exact_dot(a, b):
    return lax.dot_general(
        a,
        b,
        (((1,), (1,)), ((), ())),
        precision=lax.Precision.HIGHEST,
        preferred_element_type=jnp.float32,
    )


def flow_tables(total, parts, me, delta, kind, sending):
    send, recv, _, _ = offsets(total, parts)
    rows, place, first = [], [], []
    for i in range(parts):
        key = (i, i + delta) if sending else (i - delta, i)
        what = flows(total, parts).get(key)
        good = what is not None and what[0] == kind
        rows.append(what[2] if good else 0)
        place.append((send if sending else recv)[key] if good else 0)
        first.append(what[1] if good else 0)
    return table(me, rows), table(me, place), table(me, first)


def hops(total, parts, kind):
    return sorted({d - s for (s, d), what in flows(total, parts).items() if what[0] == kind})


def send_weights(total, parts, me, block, rows, low_ref, weight_ref):
    k, c = iota((rows, block), 0), iota((rows, block), 1)
    out = jnp.zeros((rows, block), jnp.float32)
    for delta in hops(total, parts, False):
        n, at, first = flow_tables(total, parts, me, delta, False, True)
        here = (k >= at) & (k < at + n)
        out = out + jnp.where(here & (c == k - at + first - me * block), 1.0, 0.0)
    for delta in hops(total, parts, True):
        n, at, first = flow_tables(total, parts, me, delta, True, True)
        owner = jnp.clip(me + delta, 0, parts - 1)
        low = low_ref[pl.ds(owner, 1), :] - me * block
        weight = weight_ref[pl.ds(owner, 1), :]
        row = iota((block, block), 0)
        band = jnp.where(row == low, weight, 0.0) + jnp.where(row == low + 1, 1.0 - weight, 0.0)
        pick = (k >= at) & (k < at + n) & (c == k - at + first - owner * block)
        out = out + exact_dot(jnp.where(pick, 1.0, 0.0), band)
    high, low_part = split(out)
    return jnp.concatenate([high, high, low_part], axis=1)


def pool_rows(block, level):
    o, i = iota((block >> level, block), 0), iota((block >> level, block), 1)
    return jnp.where(i >> level == o, 0.5**level, 0.0).astype(jnp.float32)


def all_hops(total, parts):
    return sorted({d - s for s, d in flows(total, parts)})


def coarse_weights(total, parts, me, block, low_ref, weight_ref):
    out = []
    row = iota((block, block), 0)
    for delta in [0] + all_hops(total, parts):
        owner = jnp.clip(me + delta, 0, parts - 1)
        low = low_ref[pl.ds(owner, 1), :] - me * block
        weight = weight_ref[pl.ds(owner, 1), :]
        band = jnp.where(row == low, weight, 0.0) + jnp.where(row == low + 1, 1.0 - weight, 0.0)
        out.append(exact_dot(pool_rows(block, 3), band))
    high, low_part = split(jnp.concatenate(out, axis=0))
    return jnp.concatenate([high, high, low_part], axis=1)


def own_weights(total, parts, me, block, slots, low_ref, weight_ref):
    low = low_ref[pl.ds(me, 1), :]
    weight = weight_ref[pl.ds(me, 1), :]

    def rows_of(g, valid):
        out = jnp.where(valid & (g == low), weight, 0.0)
        return out + jnp.where(valid & (g == low + 1), 1.0 - weight, 0.0)

    own = iota((block, block), 0) + me * block
    k, m = iota((slots, block), 0), iota((slots, block), 1)
    far = jnp.zeros((slots, block), jnp.float32)
    for delta in hops(total, parts, False):
        n, at, first = flow_tables(total, parts, me, delta, False, False)
        far = far + rows_of(k - at + first, (k >= at) & (k < at + n))
    for delta in hops(total, parts, True):
        n, at, first = flow_tables(total, parts, me, delta, True, False)
        here = (k >= at) & (k < at + n) & (m == k - at + first - me * block)
        far = far + jnp.where(here, 1.0, 0.0)
    band = jnp.concatenate([rows_of(own, own >= 0), far], axis=0)
    pools = [pool_rows(block, level) for level in range(4)]
    high, low_part = split(exact_dot(jnp.concatenate(pools, axis=0), band))
    return jnp.concatenate([high, high, low_part], axis=1)


def columns(j, size):
    return pl.ds(pl.multiple_of(j * size, size), size)


def triple(x):
    high, low_part = split(x)
    return jnp.concatenate([high, low_part, high], axis=0)


def dot(a, b):
    return jnp.dot(a, b, preferred_element_type=jnp.float32)


def chunk_rows(total, parts, j, own, recv, in_w, levels):
    block, (chunks, slots) = own.shape[0], recv.shape[:2]
    got = table(lax.axis_index("rows"), offsets(total, parts)[3])
    rows = recv.reshape(chunks, slots * SUB, LANES)
    row = iota((slots, LANES), 0)
    far = [
        jnp.where(row < got, rows[j, pl.ds(b, slots, stride=SUB), :], 0.0) for b in range(SUB)
    ]
    x = jnp.concatenate([own[:, columns(j, WIDE)], jnp.concatenate(far, axis=1)], axis=0)
    y = dot(in_w[: 2 * block - (block >> levels), :], triple(x))
    out, at = [], 0
    for level in range(levels + 1):
        out.append(y[at : at + (block >> level)])
        at += block >> level
    return out


def fused_kernel(
    total, parts, owners,
    low_hbm, weight_hbm, source_ref,
    merc_ref, one_ref, two_ref, rows_ref, pooled_ref, own, recv, in_w,
    low_ref, weight_ref, sent, held, three, landed, out_w, coarse_w, early, hint,
    small_sem, own_sem, send_sem, recv_sem, held_sem, early_send, early_recv, share_sem,
):
    block, width = source_ref.shape
    chunks = width // WIDE
    me, col = lax.axis_index("rows"), lax.axis_index("cols")
    groups = legs(total, parts)
    _, _, rows_out, rows_in = offsets(total, parts)
    slots = recv.shape[1]
    send_rows = sent.shape[1]
    each = three.shape[1]
    hop_list = all_hops(total, parts)

    loads = [
        pltpu.make_async_copy(source_ref.at[:, at], own.at[:, at], own_sem.at[i])
        for i, at in enumerate((pl.ds(0, WIDE), pl.ds(WIDE, width - WIDE)))
    ]

    small = [
        pltpu.make_async_copy(low_hbm, low_ref, small_sem.at[0]),
        pltpu.make_async_copy(weight_hbm, weight_ref, small_sem.at[1]),
    ]
    for c in small:
        c.start()
    loads[0].start()

    def by_device(chosen, act, where):
        for i in range(parts):
            mine = [leg for leg in chosen if leg[where] == i]

            if mine:
                @pl.when(me == i)
                def _():
                    for leg in mine:
                        act(leg)

    barrier = pltpu.get_barrier_semaphore()
    ties = [leg[:2] for leg in groups] + list(flows(total, parts))
    met = [sorted({a[1 - k] for a in ties for k in (0, 1) if a[k] == i}) for i in range(parts)]
    for i in range(parts):
        @pl.when(me == i)
        def _():
            for other in met[i]:
                pl.semaphore_signal(barrier, inc=1, device_id={"rows": other}, device_id_type=MESH)

    for i in range(1, owners):
        pl.semaphore_signal(
            barrier, inc=1, device_id={"cols": lax.rem(col + i, owners)}, device_id_type=MESH
        )
    waits = [len(met[i]) + owners - 1 for i in range(parts)]

    loads[1].start()

    def copy(leg, j):
        _, target, relayed, to_relay, at, to, n, half = leg
        src, dst = (held if relayed else sent), (held if to_relay else recv)
        return pltpu.make_async_remote_copy(
            src_ref=src.at[j, pl.ds(at, n)],
            dst_ref=dst.at[j, pl.ds(to, n)],
            send_sem=send_sem.at[int(relayed)],
            recv_sem=held_sem.at[half, j] if to_relay else recv_sem.at[j],
            device_id={"rows": target},
            device_id_type=MESH,
        )

    def leave(chosen, j):
        by_device(chosen, lambda leg: copy(leg, j).start(), 0)

    def hint_copy(flow):
        k = hop_list.index(flow[1] - flow[0])
        return pltpu.make_async_remote_copy(
            src_ref=early.at[k],
            dst_ref=hint.at[k],
            send_sem=early_send.at[k],
            recv_sem=early_recv.at[k],
            device_id={"rows": flow[1]},
            device_id_type=MESH,
        )

    first_hop = [leg for leg in groups if not leg[2]]
    at_relay = [
        (a, b)
        for a in groups
        for b in groups
        if a[3] and b[2] and a[1] == b[0] and a[5] == b[4] and a[6] == b[6]
    ]

    for c in small:
        c.wait()
    out_w[...] = send_weights(total, parts, me, block, send_rows, low_ref, weight_ref)
    sent_rows = sent.reshape(chunks, send_rows * SUB, LANES)

    def prepare(j):
        y = dot(out_w[...], triple(own[:, columns(j, WIDE)]))
        for b in range(SUB):
            sent_rows[j, pl.ds(b, send_rows, stride=SUB), :] = y[:, b * LANES : (b + 1) * LANES]

    loads[0].wait()
    prepare(0)
    pl.semaphore_wait(barrier, table(me, waits))
    leave(first_hop, 0)

    coarse_w[...] = coarse_weights(total, parts, me, block, low_ref, weight_ref)
    last, known = chunks - 1, chunks - HINTED
    eighth = block >> 3
    loads[1].wait()
    for h in range(HINTED):
        y = pool_columns(dot(coarse_w[...], triple(own[:, columns(known + h, WIDE)])), 3)
        at = pl.ds(h * (WIDE >> 3), WIDE >> 3)
        for k in range(len(hop_list)):
            early[k, :, at] = y[(k + 1) * eighth : (k + 2) * eighth]
        for i in range(owners):
            three[i, :, columns(known + h, WIDE >> 3)] = y[i * each : (i + 1) * each]
    by_device(sorted(flows(total, parts)), lambda flow: hint_copy(flow).start(), 0)

    @pl.loop(1, chunks)
    def _(j):
        prepare(j)
        leave(first_hop, j)

    in_w[...] = own_weights(total, parts, me, block, slots, low_ref, weight_ref)

    def forward(j):
        def act(pair):
            copy(pair[0], j).wait_recv()
            copy(pair[1], j).start()

        for i in range(parts):
            mine = [pair for pair in at_relay if pair[1][0] == i]

            if mine:
                @pl.when(me == i)
                def _():
                    for pair in mine:
                        act(pair)

    def whole(ref, sem):
        return pltpu.make_async_remote_copy(
            src_ref=ref,
            dst_ref=ref,
            send_sem=sem,
            recv_sem=sem,
            device_id={"cols": lax.rem(col + 1, owners)},
            device_id_type=MESH,
        )

    def arrive(j):
        for i in range(parts):
            if rows_in[i]:
                @pl.when(me == i)
                def _():
                    whole(recv.at[j, pl.ds(0, rows_in[i])], recv_sem.at[j]).wait_recv()

    forward(0)

    def compute(j, levels):
        rows = chunk_rows(total, parts, j, own, recv, in_w, levels)
        merc_ref[:, columns(j, WIDE)] = rows[0]
        for level, ref in ((1, one_ref), (2, two_ref)):
            ref[:, columns(j, WIDE >> level)] = pool_columns(rows[level], level)
        if levels == 3:
            pooled = pool_columns(rows[3], 3)
            for i in range(owners):
                three[i, :, columns(j, WIDE >> 3)] = pooled[i * each : (i + 1) * each]

    @pl.loop(0, known)
    def _(j):
        forward(j + 1)
        arrive(j)
        compute(j, 3)

    by_device(sorted(flows(total, parts)), lambda flow: hint_copy(flow).wait_recv(), 1)
    for k, hop in enumerate(hop_list):
        there = table(me, [int((i - hop, i) in flows(total, parts)) for i in range(parts)]) > 0
        part = jnp.where(there, hint[k], 0.0)
        for i in range(owners):
            three[i, :, pl.ds(known * (WIDE >> 3), HINTED * (WIDE >> 3))] += part[i * each : (i + 1) * each]

    for i in range(1, owners):
        target = lax.rem(col + i, owners)
        pltpu.make_async_remote_copy(
            src_ref=three.at[target],
            dst_ref=landed.at[owners - i],
            send_sem=share_sem.at[0],
            recv_sem=share_sem.at[1],
            device_id={"cols": target},
            device_id_type=MESH,
        ).start()

    @pl.loop(known, last)
    def _(j):
        forward(j + 1)
        arrive(j)
        compute(j, 2)

    landed[0] = three[col]
    others = landed.at[pl.ds(1, owners - 1)]
    whole(others, share_sem.at[1]).wait_recv()
    finish(owners, col, landed, rows_ref, pooled_ref)
    whole(others, share_sem.at[0]).wait_send()
    by_device(sorted(flows(total, parts)), lambda flow: hint_copy(flow).wait_send(), 0)
    arrive(last)
    for i in range(parts):
        held_rows = sum(leg[6] for leg in groups if leg[2] and leg[0] == i)

        @pl.when(me == i)
        def _():
            if rows_out[i]:
                whole(sent.at[:, pl.ds(0, rows_out[i])], send_sem.at[0]).wait_send()
            if held_rows:
                whole(held.at[:, pl.ds(0, held_rows)], send_sem.at[1]).wait_send()


def finish(owners, col, landed, rows_ref, pooled_ref):
    _, each, width = landed.shape
    pairs = each // 2
    slab = 2 * LANES
    pairing = jnp.where(
        iota((slab, LANES), 0) >> 1 == iota((slab, LANES), 1), 0.25, 0.0
    ).astype(jnp.bfloat16)
    x = jnp.concatenate([landed[lax.rem(c - col + owners, owners)] for c in range(owners)], axis=1)
    rows_ref[...] = x
    sums = jnp.concatenate(
        [x[2 * p : 2 * p + 1] + x[2 * p + 1 : 2 * p + 2] for p in range(pairs)], axis=0
    )
    count = owners * width // slab
    flat = jnp.concatenate([sums[:, k * slab : (k + 1) * slab] for k in range(count)], axis=0)
    high, low_part = split(flat)
    out = jnp.dot(high, pairing, preferred_element_type=jnp.float32)
    out = out + jnp.dot(low_part, pairing, preferred_element_type=jnp.float32)
    pooled_ref[...] = jnp.concatenate(
        [out[k * pairs : (k + 1) * pairs] for k in range(count)], axis=1
    )


def write_kernel(
    total, parts,
    merc_ref, one_ref, two_ref, rows_ref, pooled_ref, own, recv, in_w,
    merc_out, one_out, two_out, rows_out, pooled_out,
    merc_last, one_last, two_last, sems,
):
    last = own.shape[1] // WIDE - 1
    copies = []

    def put(src, dst):
        copies.append(pltpu.make_async_copy(src, dst, sems.at[len(copies)]))
        copies[-1].start()

    levels = ((merc_ref, merc_out, merc_last), (one_ref, one_out, one_last), (two_ref, two_out, two_last))
    for level, (ref, out, _) in enumerate(levels):
        early = pl.ds(0, last * (WIDE >> level))
        put(ref.at[:, early], out.at[:, early])
    put(rows_ref, rows_out)
    put(pooled_ref, pooled_out)
    rows = chunk_rows(total, parts, last, own, recv, in_w, 2)
    for level, (_, out, ref) in enumerate(levels):
        ref[...] = pool_columns(rows[level], level) if level else rows[0]
        put(ref, out.at[:, pl.ds(last * (WIDE >> level), WIDE >> level)])
    for c in copies:
        c.wait()


def body(parts, owners, source, low_row, weight_low):
    total = low_row.shape[0]
    block, width = source.shape
    _, _, sent, got = offsets(total, parts)
    send_rows, slots = up(max(sent), 16), up(max(got), 16)
    hold = max([n for by in relays(total, parts).values() for n in by.values()], default=1)
    hops_out = len(all_hops(total, parts))
    chunks = width // WIDE
    each = (block >> 3) // owners
    wide_rows = block + block // 2 + block // 4 + block // 8
    f32, bf16 = jnp.float32, jnp.bfloat16
    shapes = [(block >> k, width >> k) for k in range(3)]
    shapes += [(each, owners * (width >> 3)), (each // 2, owners * (width >> 4))]
    kept = [pltpu.VMEM(s, f32) for s in shapes]
    kept += [
        pltpu.VMEM((block, width), f32),
        pltpu.VMEM((chunks, slots, SUB, LANES), f32),
        pltpu.VMEM((wide_rows, 3 * (block + slots)), bf16),
    ]
    vmem = pl.BlockSpec(memory_space=pltpu.VMEM)
    hbm = pl.BlockSpec(memory_space=pltpu.HBM)
    dma = pltpu.SemaphoreType.DMA
    outs = pl.pallas_call(
        functools.partial(fused_kernel, total, parts, owners),
        out_shape=kept,
        in_specs=[hbm] * 3,
        out_specs=[vmem] * len(kept),
        scratch_shapes=[
            pltpu.VMEM((parts, block), jnp.int32),
            pltpu.VMEM((parts, block), f32),
            pltpu.VMEM((chunks, send_rows, SUB, LANES), f32),
            pltpu.VMEM((chunks, hold, SUB, LANES), f32),
            pltpu.VMEM((owners, each, width >> 3), f32),
            pltpu.VMEM((owners, each, width >> 3), f32),
            pltpu.VMEM((send_rows, 3 * block), bf16),
            pltpu.VMEM(((1 + hops_out) * (block >> 3), 3 * block), bf16),
            pltpu.VMEM((hops_out, block >> 3, HINTED * (WIDE >> 3)), f32),
            pltpu.VMEM((hops_out, block >> 3, HINTED * (WIDE >> 3)), f32),
            dma((2,)),
            dma((2,)),
            dma((2,)),
            dma((chunks,)),
            dma((2, chunks)),
            dma((hops_out,)),
            dma((hops_out,)),
            dma((2,)),
        ],
        compiler_params=pltpu.CompilerParams(
            collective_id=0, has_side_effects=True, vmem_limit_bytes=47 << 20
        ),
        name="reproject",
    )(low_row.reshape(parts, block), weight_low.reshape(parts, block), source)
    return pl.pallas_call(
        functools.partial(write_kernel, total, parts),
        out_shape=[jax.ShapeDtypeStruct(s, f32) for s in shapes],
        in_specs=[vmem] * len(kept),
        out_specs=[hbm] * len(shapes),
        scratch_shapes=[pltpu.VMEM((block >> k, WIDE >> k), f32) for k in range(3)]
        + [dma((len(shapes) + 3,))],
        compiler_params=pltpu.CompilerParams(vmem_limit_bytes=24 << 20),
        name="write",
    )(*outs)


def solution(mesh):
    return jax.shard_map(
        functools.partial(body, mesh.shape["rows"], mesh.shape["cols"]),
        mesh=mesh,
        in_specs=(P("rows", "cols"), P(), P()),
        out_specs=(
            P("rows", "cols"),
            P("rows", "cols"),
            P("rows", "cols"),
            P(("rows", "cols"), None),
            P(("rows", "cols"), None),
        ),
        check_vma=False,
    )
```

```python
import functools
import math

import jax
import jax.numpy as jnp
import numpy as np
from jax import lax
from jax.experimental import pallas as pl
from jax.experimental.pallas import tpu as pltpu
from jax.sharding import PartitionSpec as P

LANES = 128
SUB = 8
WIDE = SUB * LANES
JITTER = 2
HINTED = 2
MESH = pl.DeviceIdType.MESH


def table(index, values):
    out = jnp.int32(values[0])
    for i in range(1, len(values)):
        if values[i] != values[i - 1]:
            out = jnp.where(index >= i, jnp.int32(values[i]), out)
    return out


@functools.lru_cache(maxsize=None)
def windows(total):
    top = 68.0 * math.pi / 180.0
    edge = math.log(math.tan(math.pi / 4 + top / 2))
    m = np.arange(total, dtype=np.float64)
    y = edge * (1.0 - (2.0 * m + 1.0) / (2.0 * total))
    lat = 2.0 * np.arctan(np.exp(y)) - math.pi / 2
    pos = (top - lat) / top * total - 0.5
    slack = 0.01 * total / 1024
    first = np.clip(np.clip(np.floor(pos - slack), 0, total - 2) - JITTER, 0, total - 2)
    last = np.clip(np.clip(np.floor(pos + slack), 0, total - 2) + JITTER, 0, total - 2) + 1
    return first.astype(int), last.astype(int)


@functools.lru_cache(maxsize=None)
def flows(total, parts):
    first, last = windows(total)
    block = total // parts
    found = {}
    for d in range(parts):
        mine = np.arange(d * block, (d + 1) * block)
        for s in range(parts):
            low, high = s * block, (s + 1) * block
            ms = mine[(last[mine] >= low) & (first[mine] < high)]
            if s == d or not len(ms):
                continue
            a, b = max(low, int(first[ms].min())), min(high - 1, int(last[ms].max()))
            m0, n = int(ms.min()), int(ms.max() - ms.min()) + 1
            found[s, d] = (False, a, b - a + 1) if b - a + 1 <= n else (True, m0, n)
    return found


def offsets(total, parts):
    send, recv, sent, got = {}, {}, [0] * parts, [0] * parts
    for (s, d), (_, _, n) in sorted(flows(total, parts).items()):
        send[s, d], recv[s, d] = sent[s], got[d]
        sent[s] += n
        got[d] += n
    return send, recv, sent, got


@functools.lru_cache(maxsize=None)
def relays(total, parts):
    moves = {k: n for k, (_, _, n) in flows(total, parts).items()}
    pairs = parts // 2
    if parts % 2 or min((d - s for s, d in moves), default=1) < 1 or max((d - s for s, d in moves), default=0) > 2:
        return {}
    plan, taken = {}, set()
    load = [moves.get((2 * z, 2 * z + 1), 0) for z in range(pairs)]
    across = 0.0
    mean = sum(load) / pairs
    for z in range(pairs - 1):
        across += load[z] - mean
        n = int(round(abs(across)))
        at = z if across > 0 else z + 1
        key, relay = (2 * at, 2 * at + 1), 2 * at + (3 if across > 0 else -1)
        if n and n < moves.get(key, 0) and relay not in taken:
            plan.setdefault(key, {})[relay] = n
            taken.add(relay)
    back = [moves.get((2 * z + 1, 2 * z + 2), 0) for z in range(pairs - 1)]
    goal = sum(back) / pairs
    over = 0
    for z in range(pairs - 1):
        want = int(round(goal * (0.975 if z == 0 else 1.0))) - over
        n = max(0, min(want, back[z]))
        if n and 2 * z not in taken:
            plan.setdefault((2 * z + 1, 2 * z + 2), {})[2 * z] = n
            taken.add(2 * z)
            over = back[z] - n
        else:
            over = back[z]
    return plan


def halves(n):
    return [(0, n // 2), (n // 2, n - n // 2)] if n > 1 else [(0, n)]


@functools.lru_cache(maxsize=None)
def legs(total, parts):
    send, recv, _, _ = offsets(total, parts)
    found = []
    for (s, d), (_, _, n) in sorted(flows(total, parts).items()):
        at = 0
        for relay, rows in sorted(relays(total, parts).get((s, d), {}).items()):
            for half, (low, n_part) in enumerate(halves(rows)):
                found.append((s, relay, False, True, send[s, d] + at + low, low, n_part, half))
                found.append((relay, d, True, False, low, recv[s, d] + at + low, n_part, half))
            at += rows
        if n > at:
            found.append((s, d, False, False, send[s, d] + at, recv[s, d] + at, n - at, 0))
    return sorted(found, key=lambda leg: not leg[3])


def up(n, k):
    return -(-n // k) * k


def split(x):
    high = x.astype(jnp.bfloat16)
    low = (x - high.astype(jnp.float32)).astype(jnp.bfloat16)
    return high, low


def iota(shape, axis):
    return lax.broadcasted_iota(jnp.int32, shape, axis)


def pool_columns(x, levels):
    rows, width = x.shape
    slab = LANES << levels
    pairing = jnp.where(
        iota((slab, LANES), 0) >> levels == iota((slab, LANES), 1), 0.5**levels, 0.0
    ).astype(jnp.bfloat16)
    pieces = width // slab
    stacked = jnp.concatenate([x[:, k * slab : (k + 1) * slab] for k in range(pieces)], axis=0)
    high, low = split(stacked)
    out = jnp.dot(high, pairing, preferred_element_type=jnp.float32)
    out = out + jnp.dot(low, pairing, preferred_element_type=jnp.float32)
    return jnp.concatenate([out[k * rows : (k + 1) * rows] for k in range(pieces)], axis=1)


def exact_dot(a, b):
    return lax.dot_general(
        a,
        b,
        (((1,), (1,)), ((), ())),
        precision=lax.Precision.HIGHEST,
        preferred_element_type=jnp.float32,
    )


def flow_tables(total, parts, me, delta, kind, sending):
    send, recv, _, _ = offsets(total, parts)
    rows, place, first = [], [], []
    for i in range(parts):
        key = (i, i + delta) if sending else (i - delta, i)
        what = flows(total, parts).get(key)
        good = what is not None and what[0] == kind
        rows.append(what[2] if good else 0)
        place.append((send if sending else recv)[key] if good else 0)
        first.append(what[1] if good else 0)
    return table(me, rows), table(me, place), table(me, first)


def hops(total, parts, kind):
    return sorted({d - s for (s, d), what in flows(total, parts).items() if what[0] == kind})


def send_weights(total, parts, me, block, rows, low_ref, weight_ref):
    k, c = iota((rows, block), 0), iota((rows, block), 1)
    out = jnp.zeros((rows, block), jnp.float32)
    for delta in hops(total, parts, False):
        n, at, first = flow_tables(total, parts, me, delta, False, True)
        here = (k >= at) & (k < at + n)
        out = out + jnp.where(here & (c == k - at + first - me * block), 1.0, 0.0)
    for delta in hops(total, parts, True):
        n, at, first = flow_tables(total, parts, me, delta, True, True)
        owner = jnp.clip(me + delta, 0, parts - 1)
        low = low_ref[pl.ds(owner, 1), :] - me * block
        weight = weight_ref[pl.ds(owner, 1), :]
        row = iota((block, block), 0)
        band = jnp.where(row == low, weight, 0.0) + jnp.where(row == low + 1, 1.0 - weight, 0.0)
        pick = (k >= at) & (k < at + n) & (c == k - at + first - owner * block)
        out = out + exact_dot(jnp.where(pick, 1.0, 0.0), band)
    high, low_part = split(out)
    return jnp.concatenate([high, high, low_part], axis=1)


def pool_rows(block, level):
    o, i = iota((block >> level, block), 0), iota((block >> level, block), 1)
    return jnp.where(i >> level == o, 0.5**level, 0.0).astype(jnp.float32)


def all_hops(total, parts):
    return sorted({d - s for s, d in flows(total, parts)})


def coarse_weights(total, parts, me, block, low_ref, weight_ref):
    out = []
    row = iota((block, block), 0)
    for delta in [0] + all_hops(total, parts):
        owner = jnp.clip(me + delta, 0, parts - 1)
        low = low_ref[pl.ds(owner, 1), :] - me * block
        weight = weight_ref[pl.ds(owner, 1), :]
        band = jnp.where(row == low, weight, 0.0) + jnp.where(row == low + 1, 1.0 - weight, 0.0)
        out.append(exact_dot(pool_rows(block, 3), band))
    high, low_part = split(jnp.concatenate(out, axis=0))
    return jnp.concatenate([high, high, low_part], axis=1)


def own_weights(total, parts, me, block, slots, low_ref, weight_ref):
    low = low_ref[pl.ds(me, 1), :]
    weight = weight_ref[pl.ds(me, 1), :]

    def rows_of(g, valid):
        out = jnp.where(valid & (g == low), weight, 0.0)
        return out + jnp.where(valid & (g == low + 1), 1.0 - weight, 0.0)

    own = iota((block, block), 0) + me * block
    k, m = iota((slots, block), 0), iota((slots, block), 1)
    far = jnp.zeros((slots, block), jnp.float32)
    for delta in hops(total, parts, False):
        n, at, first = flow_tables(total, parts, me, delta, False, False)
        far = far + rows_of(k - at + first, (k >= at) & (k < at + n))
    for delta in hops(total, parts, True):
        n, at, first = flow_tables(total, parts, me, delta, True, False)
        here = (k >= at) & (k < at + n) & (m == k - at + first - me * block)
        far = far + jnp.where(here, 1.0, 0.0)
    band = jnp.concatenate([rows_of(own, own >= 0), far], axis=0)
    pools = [pool_rows(block, level) for level in range(4)]
    high, low_part = split(exact_dot(jnp.concatenate(pools, axis=0), band))
    return jnp.concatenate([high, high, low_part], axis=1)


def columns(j, size):
    return pl.ds(pl.multiple_of(j * size, size), size)


def triple(x):
    high, low_part = split(x)
    return jnp.concatenate([high, low_part, high], axis=0)


def dot(a, b):
    return jnp.dot(a, b, preferred_element_type=jnp.float32)


def chunk_rows(total, parts, j, own, recv, in_w, levels):
    block, (chunks, slots) = own.shape[0], recv.shape[:2]
    got = table(lax.axis_index("rows"), offsets(total, parts)[3])
    rows = recv.reshape(chunks, slots * SUB, LANES)
    row = iota((slots, LANES), 0)
    far = [
        jnp.where(row < got, rows[j, pl.ds(b, slots, stride=SUB), :], 0.0) for b in range(SUB)
    ]
    x = jnp.concatenate([own[:, columns(j, WIDE)], jnp.concatenate(far, axis=1)], axis=0)
    y = dot(in_w[: 2 * block - (block >> levels), :], triple(x))
    out, at = [], 0
    for level in range(levels + 1):
        out.append(y[at : at + (block >> level)])
        at += block >> level
    return out


def fused_kernel(
    total, parts, owners,
    low_hbm, weight_hbm, source_ref,
    merc_ref, one_ref, two_ref, rows_ref, pooled_ref, own, recv, in_w,
    low_ref, weight_ref, sent, held, three, landed, out_w, coarse_w, early, hint,
    small_sem, own_sem, send_sem, recv_sem, held_sem, early_send, early_recv, share_sem,
):
    block, width = source_ref.shape
    chunks = width // WIDE
    me, col = lax.axis_index("rows"), lax.axis_index("cols")
    groups = legs(total, parts)
    _, _, rows_out, rows_in = offsets(total, parts)
    slots = recv.shape[1]
    send_rows = sent.shape[1]
    each = three.shape[1]
    hop_list = all_hops(total, parts)

    loads = [
        pltpu.make_async_copy(source_ref.at[:, at], own.at[:, at], own_sem.at[i])
        for i, at in enumerate((pl.ds(0, WIDE), pl.ds(WIDE, width - WIDE)))
    ]

    small = [
        pltpu.make_async_copy(low_hbm, low_ref, small_sem.at[0]),
        pltpu.make_async_copy(weight_hbm, weight_ref, small_sem.at[1]),
    ]
    for c in small:
        c.start()
    loads[0].start()

    def by_device(chosen, act, where):
        for i in range(parts):
            mine = [leg for leg in chosen if leg[where] == i]

            if mine:
                @pl.when(me == i)
                def _():
                    for leg in mine:
                        act(leg)

    barrier = pltpu.get_barrier_semaphore()
    ties = [leg[:2] for leg in groups] + list(flows(total, parts))
    met = [sorted({a[1 - k] for a in ties for k in (0, 1) if a[k] == i}) for i in range(parts)]
    for i in range(parts):
        @pl.when(me == i)
        def _():
            for other in met[i]:
                pl.semaphore_signal(barrier, inc=1, device_id={"rows": other}, device_id_type=MESH)

    for i in range(1, owners):
        pl.semaphore_signal(
            barrier, inc=1, device_id={"cols": lax.rem(col + i, owners)}, device_id_type=MESH
        )
    waits = [len(met[i]) + owners - 1 for i in range(parts)]

    loads[1].start()

    def copy(leg, j):
        _, target, relayed, to_relay, at, to, n, half = leg
        src, dst = (held if relayed else sent), (held if to_relay else recv)
        return pltpu.make_async_remote_copy(
            src_ref=src.at[j, pl.ds(at, n)],
            dst_ref=dst.at[j, pl.ds(to, n)],
            send_sem=send_sem.at[int(relayed)],
            recv_sem=held_sem.at[half, j] if to_relay else recv_sem.at[j],
            device_id={"rows": target},
            device_id_type=MESH,
        )

    def leave(chosen, j):
        by_device(chosen, lambda leg: copy(leg, j).start(), 0)

    def hint_copy(flow):
        k = hop_list.index(flow[1] - flow[0])
        return pltpu.make_async_remote_copy(
            src_ref=early.at[k],
            dst_ref=hint.at[k],
            send_sem=early_send.at[k],
            recv_sem=early_recv.at[k],
            device_id={"rows": flow[1]},
            device_id_type=MESH,
        )

    first_hop = [leg for leg in groups if not leg[2]]
    at_relay = [
        (a, b)
        for a in groups
        for b in groups
        if a[3] and b[2] and a[1] == b[0] and a[5] == b[4] and a[6] == b[6]
    ]

    for c in small:
        c.wait()
    out_w[...] = send_weights(total, parts, me, block, send_rows, low_ref, weight_ref)
    sent_rows = sent.reshape(chunks, send_rows * SUB, LANES)

    def prepare(j):
        y = dot(out_w[...], triple(own[:, columns(j, WIDE)]))
        for b in range(SUB):
            sent_rows[j, pl.ds(b, send_rows, stride=SUB), :] = y[:, b * LANES : (b + 1) * LANES]

    loads[0].wait()
    prepare(0)
    pl.semaphore_wait(barrier, table(me, waits))
    leave(first_hop, 0)

    coarse_w[...] = coarse_weights(total, parts, me, block, low_ref, weight_ref)
    last, known = chunks - 1, chunks - HINTED
    eighth = block >> 3
    loads[1].wait()
    for h in range(HINTED):
        y = pool_columns(dot(coarse_w[...], triple(own[:, columns(known + h, WIDE)])), 3)
        at = pl.ds(h * (WIDE >> 3), WIDE >> 3)
        for k in range(len(hop_list)):
            early[k, :, at] = y[(k + 1) * eighth : (k + 2) * eighth]
        for i in range(owners):
            three[i, :, columns(known + h, WIDE >> 3)] = y[i * each : (i + 1) * each]
    by_device(sorted(flows(total, parts)), lambda flow: hint_copy(flow).start(), 0)

    @pl.loop(1, chunks)
    def _(j):
        prepare(j)
        leave(first_hop, j)

    in_w[...] = own_weights(total, parts, me, block, slots, low_ref, weight_ref)

    def forward(j, soon):
        def act(pair):
            copy(pair[0], j).wait_recv()
            copy(pair[1], j).start()

        for i in range(parts):
            mine = [
                (a, b) for a, b in at_relay if b[0] == i and (a[0] // 2 == b[1] // 2) == soon
            ]

            if mine:
                @pl.when(me == i)
                def _():
                    for pair in mine:
                        act(pair)

    def whole(ref, sem):
        return pltpu.make_async_remote_copy(
            src_ref=ref,
            dst_ref=ref,
            send_sem=sem,
            recv_sem=sem,
            device_id={"cols": lax.rem(col + 1, owners)},
            device_id_type=MESH,
        )

    def arrive(j):
        for i in range(parts):
            if rows_in[i]:
                @pl.when(me == i)
                def _():
                    whole(recv.at[j, pl.ds(0, rows_in[i])], recv_sem.at[j]).wait_recv()

    @pl.loop(0, chunks)
    def _(j):
        forward(j, True)

    forward(0, False)

    def compute(j, levels):
        rows = chunk_rows(total, parts, j, own, recv, in_w, levels)
        merc_ref[:, columns(j, WIDE)] = rows[0]
        for level, ref in ((1, one_ref), (2, two_ref)):
            ref[:, columns(j, WIDE >> level)] = pool_columns(rows[level], level)
        if levels == 3:
            pooled = pool_columns(rows[3], 3)
            for i in range(owners):
                three[i, :, columns(j, WIDE >> 3)] = pooled[i * each : (i + 1) * each]

    @pl.loop(0, known)
    def _(j):
        forward(j + 1, False)
        arrive(j)
        compute(j, 3)

    by_device(sorted(flows(total, parts)), lambda flow: hint_copy(flow).wait_recv(), 1)
    for k, hop in enumerate(hop_list):
        there = table(me, [int((i - hop, i) in flows(total, parts)) for i in range(parts)]) > 0
        part = jnp.where(there, hint[k], 0.0)
        for i in range(owners):
            three[i, :, pl.ds(known * (WIDE >> 3), HINTED * (WIDE >> 3))] += part[i * each : (i + 1) * each]

    for i in range(1, owners):
        target = lax.rem(col + i, owners)
        pltpu.make_async_remote_copy(
            src_ref=three.at[target],
            dst_ref=landed.at[owners - i],
            send_sem=share_sem.at[0],
            recv_sem=share_sem.at[1],
            device_id={"cols": target},
            device_id_type=MESH,
        ).start()

    @pl.loop(known, last)
    def _(j):
        forward(j + 1, False)
        arrive(j)
        compute(j, 2)

    landed[0] = three[col]
    others = landed.at[pl.ds(1, owners - 1)]
    whole(others, share_sem.at[1]).wait_recv()
    finish(owners, col, landed, rows_ref, pooled_ref)
    whole(others, share_sem.at[0]).wait_send()
    by_device(sorted(flows(total, parts)), lambda flow: hint_copy(flow).wait_send(), 0)
    arrive(last)
    for i in range(parts):
        held_rows = sum(leg[6] for leg in groups if leg[2] and leg[0] == i)

        @pl.when(me == i)
        def _():
            if rows_out[i]:
                whole(sent.at[:, pl.ds(0, rows_out[i])], send_sem.at[0]).wait_send()
            if held_rows:
                whole(held.at[:, pl.ds(0, held_rows)], send_sem.at[1]).wait_send()


def finish(owners, col, landed, rows_ref, pooled_ref):
    _, each, width = landed.shape
    pairs = each // 2
    slab = 2 * LANES
    pairing = jnp.where(
        iota((slab, LANES), 0) >> 1 == iota((slab, LANES), 1), 0.25, 0.0
    ).astype(jnp.bfloat16)
    x = jnp.concatenate([landed[lax.rem(c - col + owners, owners)] for c in range(owners)], axis=1)
    rows_ref[...] = x
    sums = jnp.concatenate(
        [x[2 * p : 2 * p + 1] + x[2 * p + 1 : 2 * p + 2] for p in range(pairs)], axis=0
    )
    count = owners * width // slab
    flat = jnp.concatenate([sums[:, k * slab : (k + 1) * slab] for k in range(count)], axis=0)
    high, low_part = split(flat)
    out = jnp.dot(high, pairing, preferred_element_type=jnp.float32)
    out = out + jnp.dot(low_part, pairing, preferred_element_type=jnp.float32)
    pooled_ref[...] = jnp.concatenate(
        [out[k * pairs : (k + 1) * pairs] for k in range(count)], axis=1
    )


def write_kernel(
    total, parts,
    merc_ref, one_ref, two_ref, rows_ref, pooled_ref, own, recv, in_w,
    merc_out, one_out, two_out, rows_out, pooled_out,
    merc_last, one_last, two_last, sems,
):
    last = own.shape[1] // WIDE - 1
    copies = []

    def put(src, dst):
        copies.append(pltpu.make_async_copy(src, dst, sems.at[len(copies)]))
        copies[-1].start()

    levels = ((merc_ref, merc_out, merc_last), (one_ref, one_out, one_last), (two_ref, two_out, two_last))
    for level, (ref, out, _) in enumerate(levels):
        early = pl.ds(0, last * (WIDE >> level))
        put(ref.at[:, early], out.at[:, early])
    put(rows_ref, rows_out)
    put(pooled_ref, pooled_out)
    rows = chunk_rows(total, parts, last, own, recv, in_w, 2)
    for level, (_, out, ref) in enumerate(levels):
        ref[...] = pool_columns(rows[level], level) if level else rows[0]
        put(ref, out.at[:, pl.ds(last * (WIDE >> level), WIDE >> level)])
    for c in copies:
        c.wait()


def body(parts, owners, source, low_row, weight_low):
    total = low_row.shape[0]
    block, width = source.shape
    _, _, sent, got = offsets(total, parts)
    send_rows, slots = up(max(sent), 16), up(max(got), 16)
    hold = max([n for by in relays(total, parts).values() for n in by.values()], default=1)
    hops_out = len(all_hops(total, parts))
    chunks = width // WIDE
    each = (block >> 3) // owners
    wide_rows = block + block // 2 + block // 4 + block // 8
    f32, bf16 = jnp.float32, jnp.bfloat16
    shapes = [(block >> k, width >> k) for k in range(3)]
    shapes += [(each, owners * (width >> 3)), (each // 2, owners * (width >> 4))]
    kept = [pltpu.VMEM(s, f32) for s in shapes]
    kept += [
        pltpu.VMEM((block, width), f32),
        pltpu.VMEM((chunks, slots, SUB, LANES), f32),
        pltpu.VMEM((wide_rows, 3 * (block + slots)), bf16),
    ]
    vmem = pl.BlockSpec(memory_space=pltpu.VMEM)
    hbm = pl.BlockSpec(memory_space=pltpu.HBM)
    dma = pltpu.SemaphoreType.DMA
    outs = pl.pallas_call(
        functools.partial(fused_kernel, total, parts, owners),
        out_shape=kept,
        in_specs=[hbm] * 3,
        out_specs=[vmem] * len(kept),
        scratch_shapes=[
            pltpu.VMEM((parts, block), jnp.int32),
            pltpu.VMEM((parts, block), f32),
            pltpu.VMEM((chunks, send_rows, SUB, LANES), f32),
            pltpu.VMEM((chunks, hold, SUB, LANES), f32),
            pltpu.VMEM((owners, each, width >> 3), f32),
            pltpu.VMEM((owners, each, width >> 3), f32),
            pltpu.VMEM((send_rows, 3 * block), bf16),
            pltpu.VMEM(((1 + hops_out) * (block >> 3), 3 * block), bf16),
            pltpu.VMEM((hops_out, block >> 3, HINTED * (WIDE >> 3)), f32),
            pltpu.VMEM((hops_out, block >> 3, HINTED * (WIDE >> 3)), f32),
            dma((2,)),
            dma((2,)),
            dma((2,)),
            dma((chunks,)),
            dma((2, chunks)),
            dma((hops_out,)),
            dma((hops_out,)),
            dma((2,)),
        ],
        compiler_params=pltpu.CompilerParams(
            collective_id=0, has_side_effects=True, vmem_limit_bytes=47 << 20
        ),
        name="reproject",
    )(low_row.reshape(parts, block), weight_low.reshape(parts, block), source)
    return pl.pallas_call(
        functools.partial(write_kernel, total, parts),
        out_shape=[jax.ShapeDtypeStruct(s, f32) for s in shapes],
        in_specs=[vmem] * len(kept),
        out_specs=[hbm] * len(shapes),
        scratch_shapes=[pltpu.VMEM((block >> k, WIDE >> k), f32) for k in range(3)]
        + [dma((len(shapes) + 3,))],
        compiler_params=pltpu.CompilerParams(vmem_limit_bytes=24 << 20),
        name="write",
    )(*outs)


def solution(mesh):
    return jax.shard_map(
        functools.partial(body, mesh.shape["rows"], mesh.shape["cols"]),
        mesh=mesh,
        in_specs=(P("rows", "cols"), P(), P()),
        out_specs=(
            P("rows", "cols"),
            P("rows", "cols"),
            P("rows", "cols"),
            P(("rows", "cols"), None),
            P(("rows", "cols"), None),
        ),
        check_vma=False,
    )
```

```python
import functools
import math

import jax
import jax.numpy as jnp
import numpy as np
from jax import lax
from jax.experimental import pallas as pl
from jax.experimental.pallas import tpu as pltpu
from jax.sharding import PartitionSpec as P

LANES = 128
SUB = 8
WIDE = SUB * LANES
JITTER = 2
HINTED = 2
MESH = pl.DeviceIdType.MESH


def table(index, values):
    out = jnp.int32(values[0])
    for i in range(1, len(values)):
        if values[i] != values[i - 1]:
            out = jnp.where(index >= i, jnp.int32(values[i]), out)
    return out


@functools.lru_cache(maxsize=None)
def windows(total):
    top = 68.0 * math.pi / 180.0
    edge = math.log(math.tan(math.pi / 4 + top / 2))
    m = np.arange(total, dtype=np.float64)
    y = edge * (1.0 - (2.0 * m + 1.0) / (2.0 * total))
    lat = 2.0 * np.arctan(np.exp(y)) - math.pi / 2
    pos = (top - lat) / top * total - 0.5
    slack = 0.01 * total / 1024
    first = np.clip(np.clip(np.floor(pos - slack), 0, total - 2) - JITTER, 0, total - 2)
    last = np.clip(np.clip(np.floor(pos + slack), 0, total - 2) + JITTER, 0, total - 2) + 1
    return first.astype(int), last.astype(int)


@functools.lru_cache(maxsize=None)
def flows(total, parts):
    first, last = windows(total)
    block = total // parts
    found = {}
    for d in range(parts):
        mine = np.arange(d * block, (d + 1) * block)
        for s in range(parts):
            low, high = s * block, (s + 1) * block
            ms = mine[(last[mine] >= low) & (first[mine] < high)]
            if s == d or not len(ms):
                continue
            a, b = max(low, int(first[ms].min())), min(high - 1, int(last[ms].max()))
            m0, n = int(ms.min()), int(ms.max() - ms.min()) + 1
            found[s, d] = (False, a, b - a + 1) if b - a + 1 <= n else (True, m0, n)
    return found


def offsets(total, parts):
    send, recv, sent, got = {}, {}, [0] * parts, [0] * parts
    for (s, d), (_, _, n) in sorted(flows(total, parts).items()):
        send[s, d], recv[s, d] = sent[s], got[d]
        sent[s] += n
        got[d] += n
    return send, recv, sent, got


@functools.lru_cache(maxsize=None)
def relays(total, parts):
    moves = {k: n for k, (_, _, n) in flows(total, parts).items()}
    pairs = parts // 2
    if parts % 2 or min((d - s for s, d in moves), default=1) < 1 or max((d - s for s, d in moves), default=0) > 2:
        return {}
    plan, taken = {}, set()
    load = [moves.get((2 * z, 2 * z + 1), 0) for z in range(pairs)]
    across = 0.0
    mean = sum(load) / pairs
    for z in range(pairs - 1):
        across += load[z] - mean
        n = int(round(abs(across)))
        at = z if across > 0 else z + 1
        key, relay = (2 * at, 2 * at + 1), 2 * at + (3 if across > 0 else -1)
        if n and n < moves.get(key, 0) and relay not in taken:
            plan.setdefault(key, {})[relay] = n
            taken.add(relay)
    back = [moves.get((2 * z + 1, 2 * z + 2), 0) for z in range(pairs - 1)]
    goal = sum(back) / pairs
    over = 0
    for z in range(pairs - 1):
        want = int(round(goal * (0.975 if z == 0 else 1.0))) - over
        n = max(0, min(want, back[z]))
        if n and 2 * z not in taken:
            plan.setdefault((2 * z + 1, 2 * z + 2), {})[2 * z] = n
            taken.add(2 * z)
            over = back[z] - n
        else:
            over = back[z]
    return plan


def near(i, j):
    return i // 2 == j // 2 or abs(i - j) == 2


def halves(n):
    return [(0, n // 2), (n // 2, n - n // 2)] if n > 1 else [(0, n)]


@functools.lru_cache(maxsize=None)
def legs(total, parts):
    send, recv, _, _ = offsets(total, parts)
    found = []
    for (s, d), (_, _, n) in sorted(flows(total, parts).items()):
        at = 0
        for relay, rows in sorted(relays(total, parts).get((s, d), {}).items()):
            for half, (low, n_part) in enumerate(halves(rows)):
                found.append((s, relay, False, True, send[s, d] + at + low, low, n_part, half))
                found.append((relay, d, True, False, low, recv[s, d] + at + low, n_part, half))
            at += rows
        if n > at:
            found.append((s, d, False, False, send[s, d] + at, recv[s, d] + at, n - at, 0))
    return sorted(found, key=lambda leg: not leg[3])


def up(n, k):
    return -(-n // k) * k


def split(x):
    high = x.astype(jnp.bfloat16)
    low = (x - high.astype(jnp.float32)).astype(jnp.bfloat16)
    return high, low


def iota(shape, axis):
    return lax.broadcasted_iota(jnp.int32, shape, axis)


def pool_columns(x, levels):
    rows, width = x.shape
    slab = LANES << levels
    pairing = jnp.where(
        iota((slab, LANES), 0) >> levels == iota((slab, LANES), 1), 0.5**levels, 0.0
    ).astype(jnp.bfloat16)
    pieces = width // slab
    stacked = jnp.concatenate([x[:, k * slab : (k + 1) * slab] for k in range(pieces)], axis=0)
    high, low = split(stacked)
    out = jnp.dot(high, pairing, preferred_element_type=jnp.float32)
    out = out + jnp.dot(low, pairing, preferred_element_type=jnp.float32)
    return jnp.concatenate([out[k * rows : (k + 1) * rows] for k in range(pieces)], axis=1)


def exact_dot(a, b):
    return lax.dot_general(
        a,
        b,
        (((1,), (1,)), ((), ())),
        precision=lax.Precision.HIGHEST,
        preferred_element_type=jnp.float32,
    )


def flow_tables(total, parts, me, delta, kind, sending):
    send, recv, _, _ = offsets(total, parts)
    rows, place, first = [], [], []
    for i in range(parts):
        key = (i, i + delta) if sending else (i - delta, i)
        what = flows(total, parts).get(key)
        good = what is not None and what[0] == kind
        rows.append(what[2] if good else 0)
        place.append((send if sending else recv)[key] if good else 0)
        first.append(what[1] if good else 0)
    return table(me, rows), table(me, place), table(me, first)


def hops(total, parts, kind):
    return sorted({d - s for (s, d), what in flows(total, parts).items() if what[0] == kind})


def send_weights(total, parts, me, block, rows, low_ref, weight_ref):
    k, c = iota((rows, block), 0), iota((rows, block), 1)
    high = jnp.zeros((rows, block), jnp.float32)
    low_part = high
    for delta in hops(total, parts, False):
        n, at, first = flow_tables(total, parts, me, delta, False, True)
        here = (k >= at) & (k < at + n)
        high = high + jnp.where(here & (c == k - at + first - me * block), 1.0, 0.0)
    for delta in hops(total, parts, True):
        n, at, first = flow_tables(total, parts, me, delta, True, True)
        owner = jnp.clip(me + delta, 0, parts - 1)
        low = low_ref[pl.ds(owner, 1), :] - me * block
        weight = weight_ref[pl.ds(owner, 1), :]
        row = iota((block, block), 0)
        band = jnp.where(row == low, weight, 0.0) + jnp.where(row == low + 1, 1.0 - weight, 0.0)
        pick = (k >= at) & (k < at + n) & (c == k - at + first - owner * block)
        both = lax.dot_general(
            jnp.where(pick, 1.0, 0.0).astype(jnp.bfloat16),
            jnp.concatenate(split(band), axis=0),
            (((1,), (1,)), ((), ())),
            preferred_element_type=jnp.float32,
        )
        high, low_part = high + both[:, :block], low_part + both[:, block:]
    high, low_part = high.astype(jnp.bfloat16), low_part.astype(jnp.bfloat16)
    return jnp.concatenate([high, high, low_part], axis=1)


def pool_rows(block, level):
    o, i = iota((block >> level, block), 0), iota((block >> level, block), 1)
    return jnp.where(i >> level == o, 0.5**level, 0.0).astype(jnp.float32)


def all_hops(total, parts):
    return sorted({d - s for s, d in flows(total, parts)})


def coarse_weights(total, parts, me, block, low_ref, weight_ref):
    out = []
    row = iota((block, block), 0)
    for delta in [0] + all_hops(total, parts):
        owner = jnp.clip(me + delta, 0, parts - 1)
        low = low_ref[pl.ds(owner, 1), :] - me * block
        weight = weight_ref[pl.ds(owner, 1), :]
        band = jnp.where(row == low, weight, 0.0) + jnp.where(row == low + 1, 1.0 - weight, 0.0)
        out.append(exact_dot(pool_rows(block, 3), band))
    high, low_part = split(jnp.concatenate(out, axis=0))
    return jnp.concatenate([high, high, low_part], axis=1)


def own_weights(total, parts, me, block, slots, low_ref, weight_ref):
    low = low_ref[pl.ds(me, 1), :]
    weight = weight_ref[pl.ds(me, 1), :]

    def rows_of(g, valid):
        out = jnp.where(valid & (g == low), weight, 0.0)
        return out + jnp.where(valid & (g == low + 1), 1.0 - weight, 0.0)

    own = iota((block, block), 0) + me * block
    k, m = iota((slots, block), 0), iota((slots, block), 1)
    far = jnp.zeros((slots, block), jnp.float32)
    for delta in hops(total, parts, False):
        n, at, first = flow_tables(total, parts, me, delta, False, False)
        far = far + rows_of(k - at + first, (k >= at) & (k < at + n))
    for delta in hops(total, parts, True):
        n, at, first = flow_tables(total, parts, me, delta, True, False)
        here = (k >= at) & (k < at + n) & (m == k - at + first - me * block)
        far = far + jnp.where(here, 1.0, 0.0)
    band = jnp.concatenate([rows_of(own, own >= 0), far], axis=0)
    pools = [pool_rows(block, level) for level in range(4)]
    high, low_part = split(exact_dot(jnp.concatenate(pools, axis=0), band))
    return jnp.concatenate([high, high, low_part], axis=1)


def columns(j, size):
    return pl.ds(pl.multiple_of(j * size, size), size)


def triple(x):
    high, low_part = split(x)
    return jnp.concatenate([high, low_part, high], axis=0)


def dot(a, b):
    return jnp.dot(a, b, preferred_element_type=jnp.float32)


def chunk_operand(total, parts, j, own, recv):
    chunks, slots = recv.shape[:2]
    got = table(lax.axis_index("rows"), offsets(total, parts)[3])
    rows = recv.reshape(chunks, slots * SUB, LANES)
    row = iota((slots, LANES), 0)
    far = [
        jnp.where(row < got, rows[j, pl.ds(b, slots, stride=SUB), :], 0.0) for b in range(SUB)
    ]
    return triple(
        jnp.concatenate([own[:, columns(j, WIDE)], jnp.concatenate(far, axis=1)], axis=0)
    )


def chunk_rows(block, in_w, x, levels):
    at = [2 * block - (2 * block >> level) for level in levels]
    y = dot(in_w[at[0] : at[-1] + (block >> levels[-1]), :], x)
    return [y[a - at[0] : a - at[0] + (block >> level)] for a, level in zip(at, levels)]


def fused_kernel(
    total, parts, owners,
    low_hbm, weight_hbm, source_ref,
    merc_ref, one_ref, two_ref, rows_ref, pooled_ref, own, recv, in_w,
    low_ref, weight_ref, sent, held, three, landed, out_w, coarse_w, early, hint,
    small_sem, own_sem, send_sem, recv_sem, held_sem, early_send, early_recv, share_sem, met_sem,
):
    block, width = source_ref.shape
    chunks = width // WIDE
    me, col = lax.axis_index("rows"), lax.axis_index("cols")
    groups = legs(total, parts)
    _, _, rows_out, rows_in = offsets(total, parts)
    slots = recv.shape[1]
    send_rows = sent.shape[1]
    each = three.shape[1]
    hop_list = all_hops(total, parts)

    barrier = pltpu.get_barrier_semaphore()
    ties = {leg[:2] for leg in groups} | set(flows(total, parts))
    met = [[j for j in range(parts) if (i, j) in ties or (j, i) in ties] for i in range(parts)]
    stepped = bool(relays(total, parts))
    if stepped:
        met = [[j for j in range(parts) if j != i and near(i, j)] for i in range(parts)]

    def greet(sem):
        for i in range(parts):
            @pl.when(me == i)
            def _():
                for j in met[i]:
                    pl.semaphore_signal(sem, inc=1, device_id={"rows": j}, device_id_type=MESH)

    greet(barrier)
    for i in range(1, owners):
        pl.semaphore_signal(
            barrier, inc=1, device_id={"cols": lax.rem(col + i, owners)}, device_id_type=MESH
        )

    loads = [
        pltpu.make_async_copy(source_ref.at[:, at], own.at[:, at], own_sem.at[i])
        for i, at in enumerate((pl.ds(0, WIDE), pl.ds(WIDE, width - WIDE)))
    ]

    small = [
        pltpu.make_async_copy(low_hbm, low_ref, small_sem.at[0]),
        pltpu.make_async_copy(weight_hbm, weight_ref, small_sem.at[1]),
    ]
    for c in small:
        c.start()
    loads[0].start()

    def by_device(chosen, act, where):
        for i in range(parts):
            mine = [leg for leg in chosen if leg[where] == i]

            if mine:
                @pl.when(me == i)
                def _():
                    for leg in mine:
                        act(leg)

    loads[1].start()

    def copy(leg, j):
        _, target, relayed, to_relay, at, to, n, half = leg
        src, dst = (held if relayed else sent), (held if to_relay else recv)
        return pltpu.make_async_remote_copy(
            src_ref=src.at[j, pl.ds(at, n)],
            dst_ref=dst.at[j, pl.ds(to, n)],
            send_sem=send_sem.at[int(relayed)],
            recv_sem=held_sem.at[half, j] if to_relay else recv_sem.at[j],
            device_id={"rows": target},
            device_id_type=MESH,
        )

    def leave(chosen, j):
        by_device(chosen, lambda leg: copy(leg, j).start(), 0)

    def hint_copy(flow):
        k = hop_list.index(flow[1] - flow[0])
        return pltpu.make_async_remote_copy(
            src_ref=early.at[k],
            dst_ref=hint.at[k],
            send_sem=early_send.at[k],
            recv_sem=early_recv.at[k],
            device_id={"rows": flow[1]},
            device_id_type=MESH,
        )

    first_hop = [leg for leg in groups if not leg[2]]
    at_relay = [
        (a, b)
        for a in groups
        for b in groups
        if a[3] and b[2] and a[1] == b[0] and a[5] == b[4] and a[6] == b[6]
    ]

    for c in small:
        c.wait()
    out_w[...] = send_weights(total, parts, me, block, send_rows, low_ref, weight_ref)
    sent_rows = sent.reshape(chunks, send_rows * SUB, LANES)

    def prepare(j):
        y = dot(out_w[...], triple(own[:, columns(j, WIDE)]))
        for b in range(SUB):
            sent_rows[j, pl.ds(b, send_rows, stride=SUB), :] = y[:, b * LANES : (b + 1) * LANES]

    loads[0].wait()
    prepare(0)
    pl.semaphore_wait(barrier, table(me, [len(m) + owners - 1 for m in met]))
    if stepped:
        greet(met_sem)
    here = [leg for leg in first_hop if not stepped or near(*leg[:2])]
    leave(here, 0)

    coarse_w[...] = coarse_weights(total, parts, me, block, low_ref, weight_ref)
    last, known = chunks - 1, chunks - HINTED
    eighth = block >> 3
    loads[1].wait()
    for h in range(HINTED):
        y = pool_columns(dot(coarse_w[...], triple(own[:, columns(known + h, WIDE)])), 3)
        for k in range(len(hop_list)):
            early[k, :, columns(h, WIDE >> 3)] = y[(k + 1) * eighth : (k + 2) * eighth]
        for i in range(owners):
            three[i, :, columns(known + h, WIDE >> 3)] = y[i * each : (i + 1) * each]
    if stepped:
        pl.semaphore_wait(met_sem, table(me, [len(m) for m in met]))
        leave([leg for leg in first_hop if leg not in here], 0)
    by_device(sorted(flows(total, parts)), lambda flow: hint_copy(flow).start(), 0)

    @pl.loop(1, chunks)
    def _(j):
        prepare(j)
        leave(first_hop, j)

    in_w[...] = own_weights(total, parts, me, block, slots, low_ref, weight_ref)

    def forward(j, soon):
        def act(pair):
            copy(pair[0], j).wait_recv()
            copy(pair[1], j).start()

        for i in range(parts):
            mine = [
                (a, b) for a, b in at_relay if b[0] == i and (a[0] // 2 == b[1] // 2) == soon
            ]

            if mine:
                @pl.when(me == i)
                def _():
                    for pair in mine:
                        act(pair)

    def whole(ref, sem):
        return pltpu.make_async_remote_copy(
            src_ref=ref,
            dst_ref=ref,
            send_sem=sem,
            recv_sem=sem,
            device_id={"cols": lax.rem(col + 1, owners)},
            device_id_type=MESH,
        )

    def arrive(j):
        for i in range(parts):
            if rows_in[i]:
                @pl.when(me == i)
                def _():
                    whole(recv.at[j, pl.ds(0, rows_in[i])], recv_sem.at[j]).wait_recv()

    @pl.loop(0, chunks)
    def _(j):
        forward(j, True)

    forward(0, False)

    def compute(x, j):
        rows = chunk_rows(block, in_w, x, (0, 1, 2))
        merc_ref[:, columns(j, WIDE)] = rows[0]
        for level, ref in ((1, one_ref), (2, two_ref)):
            ref[:, columns(j, WIDE >> level)] = pool_columns(rows[level], level)

    def coarse(x, j):
        pooled = pool_columns(chunk_rows(block, in_w, x, (3,))[0], 3)
        for i in range(owners):
            three[i, :, columns(j, WIDE >> 3)] = pooled[i * each : (i + 1) * each]

    def receive(j):
        forward(j + 1, False)
        arrive(j)
        return chunk_operand(total, parts, j, own, recv)

    @pl.loop(0, known - 1)
    def _(j):
        x = receive(j)
        compute(x, j)
        coarse(x, j)

    by_device(sorted(flows(total, parts)), lambda flow: hint_copy(flow).wait_recv(), 1)
    for k, hop in enumerate(hop_list):
        there = table(me, [int((i - hop, i) in flows(total, parts)) for i in range(parts)]) > 0
        part = jnp.where(there, hint[k], 0.0)
        for i in range(owners):
            three[i, :, pl.ds(known * (WIDE >> 3), HINTED * (WIDE >> 3))] += part[i * each : (i + 1) * each]

    x = receive(known - 1)
    coarse(x, known - 1)
    for i in range(1, owners):
        target = lax.rem(col + i, owners)
        pltpu.make_async_remote_copy(
            src_ref=three.at[target],
            dst_ref=landed.at[owners - i],
            send_sem=share_sem.at[0],
            recv_sem=share_sem.at[1],
            device_id={"cols": target},
            device_id_type=MESH,
        ).start()
    compute(x, known - 1)

    @pl.loop(known, last)
    def _(j):
        compute(receive(j), j)

    landed[0] = three[col]
    others = landed.at[pl.ds(1, owners - 1)]
    whole(others, share_sem.at[1]).wait_recv()
    finish(owners, col, landed, rows_ref, pooled_ref)
    whole(others, share_sem.at[0]).wait_send()
    by_device(sorted(flows(total, parts)), lambda flow: hint_copy(flow).wait_send(), 0)
    arrive(last)
    for i in range(parts):
        held_rows = sum(leg[6] for leg in groups if leg[2] and leg[0] == i)

        @pl.when(me == i)
        def _():
            if rows_out[i]:
                whole(sent.at[:, pl.ds(0, rows_out[i])], send_sem.at[0]).wait_send()
            if held_rows:
                whole(held.at[:, pl.ds(0, held_rows)], send_sem.at[1]).wait_send()


def finish(owners, col, landed, rows_ref, pooled_ref):
    _, each, width = landed.shape
    pairs = each // 2
    slab = 2 * LANES
    pairing = jnp.where(
        iota((slab, LANES), 0) >> 1 == iota((slab, LANES), 1), 0.25, 0.0
    ).astype(jnp.bfloat16)
    x = jnp.concatenate([landed[lax.rem(c - col + owners, owners)] for c in range(owners)], axis=1)
    rows_ref[...] = x
    sums = jnp.concatenate(
        [x[2 * p : 2 * p + 1] + x[2 * p + 1 : 2 * p + 2] for p in range(pairs)], axis=0
    )
    count = owners * width // slab
    flat = jnp.concatenate([sums[:, k * slab : (k + 1) * slab] for k in range(count)], axis=0)
    high, low_part = split(flat)
    out = jnp.dot(high, pairing, preferred_element_type=jnp.float32)
    out = out + jnp.dot(low_part, pairing, preferred_element_type=jnp.float32)
    pooled_ref[...] = jnp.concatenate(
        [out[k * pairs : (k + 1) * pairs] for k in range(count)], axis=1
    )


def write_kernel(
    total, parts,
    merc_ref, one_ref, two_ref, rows_ref, pooled_ref, own, recv, in_w,
    merc_out, one_out, two_out, rows_out, pooled_out,
    merc_last, one_last, two_last, sems,
):
    last = own.shape[1] // WIDE - 1
    copies = []

    def put(src, dst):
        copies.append(pltpu.make_async_copy(src, dst, sems.at[len(copies)]))
        copies[-1].start()

    levels = ((merc_ref, merc_out, merc_last), (one_ref, one_out, one_last), (two_ref, two_out, two_last))
    for level, (ref, out, _) in enumerate(levels):
        early = pl.ds(0, last * (WIDE >> level))
        put(ref.at[:, early], out.at[:, early])
    put(rows_ref, rows_out)
    put(pooled_ref, pooled_out)
    x = chunk_operand(total, parts, last, own, recv)
    rows = chunk_rows(own.shape[0], in_w, x, (0, 1, 2))
    for level, (_, out, ref) in enumerate(levels):
        ref[...] = pool_columns(rows[level], level) if level else rows[0]
        put(ref, out.at[:, pl.ds(last * (WIDE >> level), WIDE >> level)])
    for c in copies:
        c.wait()


def body(parts, owners, source, low_row, weight_low):
    total = low_row.shape[0]
    block, width = source.shape
    _, _, sent, got = offsets(total, parts)
    send_rows, slots = up(max(sent), 16), up(max(got), 16)
    hold = max([n for by in relays(total, parts).values() for n in by.values()], default=1)
    hops_out = len(all_hops(total, parts))
    chunks = width // WIDE
    each = (block >> 3) // owners
    wide_rows = block + block // 2 + block // 4 + block // 8
    f32, bf16 = jnp.float32, jnp.bfloat16
    shapes = [(block >> k, width >> k) for k in range(3)]
    shapes += [(each, owners * (width >> 3)), (each // 2, owners * (width >> 4))]
    kept = [pltpu.VMEM(s, f32) for s in shapes]
    kept += [
        pltpu.VMEM((block, width), f32),
        pltpu.VMEM((chunks, slots, SUB, LANES), f32),
        pltpu.VMEM((wide_rows, 3 * (block + slots)), bf16),
    ]
    vmem = pl.BlockSpec(memory_space=pltpu.VMEM)
    hbm = pl.BlockSpec(memory_space=pltpu.HBM)
    dma = pltpu.SemaphoreType.DMA
    outs = pl.pallas_call(
        functools.partial(fused_kernel, total, parts, owners),
        out_shape=kept,
        in_specs=[hbm] * 3,
        out_specs=[vmem] * len(kept),
        scratch_shapes=[
            pltpu.VMEM((parts, block), jnp.int32),
            pltpu.VMEM((parts, block), f32),
            pltpu.VMEM((chunks, send_rows, SUB, LANES), f32),
            pltpu.VMEM((chunks, hold, SUB, LANES), f32),
            pltpu.VMEM((owners, each, width >> 3), f32),
            pltpu.VMEM((owners, each, width >> 3), f32),
            pltpu.VMEM((send_rows, 3 * block), bf16),
            pltpu.VMEM(((1 + hops_out) * (block >> 3), 3 * block), bf16),
            pltpu.VMEM((hops_out, block >> 3, HINTED * (WIDE >> 3)), f32),
            pltpu.VMEM((hops_out, block >> 3, HINTED * (WIDE >> 3)), f32),
            dma((2,)),
            dma((2,)),
            dma((2,)),
            dma((chunks,)),
            dma((2, chunks)),
            dma((hops_out,)),
            dma((hops_out,)),
            dma((2,)),
            pltpu.SemaphoreType.REGULAR,
        ],
        compiler_params=pltpu.CompilerParams(
            collective_id=0, has_side_effects=True, vmem_limit_bytes=47 << 20
        ),
        name="reproject",
    )(low_row.reshape(parts, block), weight_low.reshape(parts, block), source)
    return pl.pallas_call(
        functools.partial(write_kernel, total, parts),
        out_shape=[jax.ShapeDtypeStruct(s, f32) for s in shapes],
        in_specs=[vmem] * len(kept),
        out_specs=[hbm] * len(shapes),
        scratch_shapes=[pltpu.VMEM((block >> k, WIDE >> k), f32) for k in range(3)]
        + [dma((len(shapes) + 3,))],
        compiler_params=pltpu.CompilerParams(vmem_limit_bytes=24 << 20),
        name="write",
    )(*outs)


def solution(mesh):
    return jax.shard_map(
        functools.partial(body, mesh.shape["rows"], mesh.shape["cols"]),
        mesh=mesh,
        in_specs=(P("rows", "cols"), P(), P()),
        out_specs=(
            P("rows", "cols"),
            P("rows", "cols"),
            P("rows", "cols"),
            P(("rows", "cols"), None),
            P(("rows", "cols"), None),
        ),
        check_vma=False,
    )
```

```python
import functools
import math

import jax
import jax.numpy as jnp
import numpy as np
from jax import lax
from jax.experimental import pallas as pl
from jax.experimental.pallas import tpu as pltpu
from jax.sharding import PartitionSpec as P

LANES = 128
SUB = 8
WIDE = SUB * LANES
JITTER = 2
HINTED = 2
PIECES = 2
MESH = pl.DeviceIdType.MESH


def table(index, values):
    out = jnp.int32(values[0])
    for i in range(1, len(values)):
        if values[i] != values[i - 1]:
            out = jnp.where(index >= i, jnp.int32(values[i]), out)
    return out


@functools.lru_cache(maxsize=None)
def windows(total):
    top = 68.0 * math.pi / 180.0
    edge = math.log(math.tan(math.pi / 4 + top / 2))
    m = np.arange(total, dtype=np.float64)
    y = edge * (1.0 - (2.0 * m + 1.0) / (2.0 * total))
    lat = 2.0 * np.arctan(np.exp(y)) - math.pi / 2
    pos = (top - lat) / top * total - 0.5
    slack = 0.01 * total / 1024
    first = np.clip(np.clip(np.floor(pos - slack), 0, total - 2) - JITTER, 0, total - 2)
    last = np.clip(np.clip(np.floor(pos + slack), 0, total - 2) + JITTER, 0, total - 2) + 1
    return first.astype(int), last.astype(int)


@functools.lru_cache(maxsize=None)
def flows(total, parts):
    first, last = windows(total)
    block = total // parts
    found = {}
    for d in range(parts):
        mine = np.arange(d * block, (d + 1) * block)
        for s in range(parts):
            low, high = s * block, (s + 1) * block
            ms = mine[(last[mine] >= low) & (first[mine] < high)]
            if s == d or not len(ms):
                continue
            a, b = max(low, int(first[ms].min())), min(high - 1, int(last[ms].max()))
            m0, n = int(ms.min()), int(ms.max() - ms.min()) + 1
            found[s, d] = (False, a, b - a + 1) if b - a + 1 <= n else (True, m0, n)
    return found


def offsets(total, parts):
    send, recv, sent, got = {}, {}, [0] * parts, [0] * parts
    for (s, d), (_, _, n) in sorted(flows(total, parts).items()):
        send[s, d], recv[s, d] = sent[s], got[d]
        sent[s] += n
        got[d] += n
    return send, recv, sent, got


@functools.lru_cache(maxsize=None)
def relays(total, parts):
    moves = {k: n for k, (_, _, n) in flows(total, parts).items()}
    pairs = parts // 2
    if parts % 2 or min((d - s for s, d in moves), default=1) < 1 or max((d - s for s, d in moves), default=0) > 2:
        return {}
    plan, taken = {}, set()
    load = [moves.get((2 * z, 2 * z + 1), 0) for z in range(pairs)]
    across = 0.0
    mean = sum(load) / pairs
    for z in range(pairs - 1):
        across += load[z] - mean
        n = int(round(abs(across)))
        at = z if across > 0 else z + 1
        key, relay = (2 * at, 2 * at + 1), 2 * at + (3 if across > 0 else -1)
        if n and n < moves.get(key, 0) and relay not in taken:
            plan.setdefault(key, {})[relay] = n
            taken.add(relay)
    back = [moves.get((2 * z + 1, 2 * z + 2), 0) for z in range(pairs - 1)]
    goal = sum(back) / pairs
    over = 0
    for z in range(pairs - 1):
        want = int(round(goal * (0.975 if z == 0 else 1.0))) - over
        n = max(0, min(want, back[z]))
        if n and 2 * z not in taken:
            plan.setdefault((2 * z + 1, 2 * z + 2), {})[2 * z] = n
            taken.add(2 * z)
            over = back[z] - n
        else:
            over = back[z]
    return plan


def near(i, j):
    return i // 2 == j // 2 or abs(i - j) == 2


def halves(n):
    return [(0, n // 2), (n // 2, n - n // 2)] if n > 1 else [(0, n)]


@functools.lru_cache(maxsize=None)
def legs(total, parts):
    send, recv, _, _ = offsets(total, parts)
    found = []
    for (s, d), (_, _, n) in sorted(flows(total, parts).items()):
        at = 0
        for relay, rows in sorted(relays(total, parts).get((s, d), {}).items()):
            for half, (low, n_part) in enumerate(halves(rows)):
                found.append((s, relay, False, True, send[s, d] + at + low, low, n_part, half))
                found.append((relay, d, True, False, low, recv[s, d] + at + low, n_part, half))
            at += rows
        if n > at:
            found.append((s, d, False, False, send[s, d] + at, recv[s, d] + at, n - at, 0))
    return sorted(found, key=lambda leg: not leg[3])


def up(n, k):
    return -(-n // k) * k


def split(x):
    high = x.astype(jnp.bfloat16)
    low = (x - high.astype(jnp.float32)).astype(jnp.bfloat16)
    return high, low


def iota(shape, axis):
    return lax.broadcasted_iota(jnp.int32, shape, axis)


def pool_columns(x, levels):
    rows, width = x.shape
    slab = LANES << levels
    pairing = jnp.where(
        iota((slab, LANES), 0) >> levels == iota((slab, LANES), 1), 0.5**levels, 0.0
    ).astype(jnp.bfloat16)
    pieces = width // slab
    stacked = jnp.concatenate([x[:, k * slab : (k + 1) * slab] for k in range(pieces)], axis=0)
    high, low = split(stacked)
    out = jnp.dot(high, pairing, preferred_element_type=jnp.float32)
    out = out + jnp.dot(low, pairing, preferred_element_type=jnp.float32)
    return jnp.concatenate([out[k * rows : (k + 1) * rows] for k in range(pieces)], axis=1)


def exact_dot(a, b):
    return lax.dot_general(
        a,
        b,
        (((1,), (1,)), ((), ())),
        precision=lax.Precision.HIGHEST,
        preferred_element_type=jnp.float32,
    )


def flow_tables(total, parts, me, delta, kind, sending):
    send, recv, _, _ = offsets(total, parts)
    rows, place, first = [], [], []
    for i in range(parts):
        key = (i, i + delta) if sending else (i - delta, i)
        what = flows(total, parts).get(key)
        good = what is not None and what[0] == kind
        rows.append(what[2] if good else 0)
        place.append((send if sending else recv)[key] if good else 0)
        first.append(what[1] if good else 0)
    return table(me, rows), table(me, place), table(me, first)


def hops(total, parts, kind):
    return sorted({d - s for (s, d), what in flows(total, parts).items() if what[0] == kind})


def send_weights(total, parts, me, block, rows, low_ref, weight_ref):
    k, c = iota((rows, block), 0), iota((rows, block), 1)
    high = jnp.zeros((rows, block), jnp.float32)
    low_part = high
    for delta in hops(total, parts, False):
        n, at, first = flow_tables(total, parts, me, delta, False, True)
        here = (k >= at) & (k < at + n)
        high = high + jnp.where(here & (c == k - at + first - me * block), 1.0, 0.0)
    for delta in hops(total, parts, True):
        n, at, first = flow_tables(total, parts, me, delta, True, True)
        owner = jnp.clip(me + delta, 0, parts - 1)
        low = low_ref[pl.ds(owner, 1), :] - me * block
        weight = weight_ref[pl.ds(owner, 1), :]
        row = iota((block, block), 0)
        band = jnp.where(row == low, weight, 0.0) + jnp.where(row == low + 1, 1.0 - weight, 0.0)
        pick = (k >= at) & (k < at + n) & (c == k - at + first - owner * block)
        both = lax.dot_general(
            jnp.where(pick, 1.0, 0.0).astype(jnp.bfloat16),
            jnp.concatenate(split(band), axis=0),
            (((1,), (1,)), ((), ())),
            preferred_element_type=jnp.float32,
        )
        high, low_part = high + both[:, :block], low_part + both[:, block:]
    high, low_part = high.astype(jnp.bfloat16), low_part.astype(jnp.bfloat16)
    return jnp.concatenate([high, high, low_part], axis=1)


def pool_rows(block, level):
    o, i = iota((block >> level, block), 0), iota((block >> level, block), 1)
    return jnp.where(i >> level == o, 0.5**level, 0.0).astype(jnp.float32)


def all_hops(total, parts):
    return sorted({d - s for s, d in flows(total, parts)})


def coarse_weights(total, parts, me, block, low_ref, weight_ref):
    out = []
    row = iota((block, block), 0)
    for delta in [0] + all_hops(total, parts):
        owner = jnp.clip(me + delta, 0, parts - 1)
        low = low_ref[pl.ds(owner, 1), :] - me * block
        weight = weight_ref[pl.ds(owner, 1), :]
        band = jnp.where(row == low, weight, 0.0) + jnp.where(row == low + 1, 1.0 - weight, 0.0)
        out.append(exact_dot(pool_rows(block, 3), band))
    high, low_part = split(jnp.concatenate(out, axis=0))
    return jnp.concatenate([high, high, low_part], axis=1)


def own_weights(total, parts, me, block, slots, low_ref, weight_ref):
    low = low_ref[pl.ds(me, 1), :]
    weight = weight_ref[pl.ds(me, 1), :]

    def rows_of(g, valid):
        out = jnp.where(valid & (g == low), weight, 0.0)
        return out + jnp.where(valid & (g == low + 1), 1.0 - weight, 0.0)

    own = iota((block, block), 0) + me * block
    k, m = iota((slots, block), 0), iota((slots, block), 1)
    far = jnp.zeros((slots, block), jnp.float32)
    for delta in hops(total, parts, False):
        n, at, first = flow_tables(total, parts, me, delta, False, False)
        far = far + rows_of(k - at + first, (k >= at) & (k < at + n))
    for delta in hops(total, parts, True):
        n, at, first = flow_tables(total, parts, me, delta, True, False)
        here = (k >= at) & (k < at + n) & (m == k - at + first - me * block)
        far = far + jnp.where(here, 1.0, 0.0)
    band = jnp.concatenate([rows_of(own, own >= 0), far], axis=0)
    pools = [pool_rows(block, level) for level in range(4)]
    high, low_part = split(exact_dot(jnp.concatenate(pools, axis=0), band))
    return jnp.concatenate([high, high, low_part], axis=1)


def columns(j, size):
    return pl.ds(pl.multiple_of(j * size, size), size)


def triple(x):
    high, low_part = split(x)
    return jnp.concatenate([high, low_part, high], axis=0)


def dot(a, b):
    return jnp.dot(a, b, preferred_element_type=jnp.float32)


def chunk_operand(total, parts, j, own, recv):
    chunks, slots = recv.shape[:2]
    got = table(lax.axis_index("rows"), offsets(total, parts)[3])
    rows = recv.reshape(chunks, slots * SUB, LANES)
    row = iota((slots, LANES), 0)
    far = [
        jnp.where(row < got, rows[j, pl.ds(b, slots, stride=SUB), :], 0.0) for b in range(SUB)
    ]
    return triple(
        jnp.concatenate([own[:, columns(j, WIDE)], jnp.concatenate(far, axis=1)], axis=0)
    )


def chunk_rows(block, in_w, x, levels):
    at = [2 * block - (2 * block >> level) for level in levels]
    y = dot(in_w[at[0] : at[-1] + (block >> levels[-1]), :], x)
    return [y[a - at[0] : a - at[0] + (block >> level)] for a, level in zip(at, levels)]


def fused_kernel(
    total, parts, owners,
    low_hbm, weight_hbm, source_ref,
    merc_ref, one_ref, two_ref, rows_ref, pooled_ref, own, recv, in_w,
    low_ref, weight_ref, sent, held, three, landed, out_w, coarse_w, early, hint,
    small_sem, own_sem, send_sem, recv_sem, held_sem, early_send, early_recv, share_sem, met_sem,
):
    block, width = source_ref.shape
    chunks = width // WIDE
    me, col = lax.axis_index("rows"), lax.axis_index("cols")
    groups = legs(total, parts)
    _, _, rows_out, rows_in = offsets(total, parts)
    slots = recv.shape[1]
    send_rows = sent.shape[1]
    each = three.shape[1]
    hop_list = all_hops(total, parts)

    barrier = pltpu.get_barrier_semaphore()
    ties = {leg[:2] for leg in groups} | set(flows(total, parts))
    met = [[j for j in range(parts) if (i, j) in ties or (j, i) in ties] for i in range(parts)]
    stepped = bool(relays(total, parts))
    if stepped:
        met = [[j for j in range(parts) if j != i and near(i, j)] for i in range(parts)]

    def greet(sem):
        for i in range(parts):
            @pl.when(me == i)
            def _():
                for j in met[i]:
                    pl.semaphore_signal(sem, inc=1, device_id={"rows": j}, device_id_type=MESH)

    greet(barrier)
    for i in range(1, owners):
        pl.semaphore_signal(
            barrier, inc=1, device_id={"cols": lax.rem(col + i, owners)}, device_id_type=MESH
        )

    loads = [
        pltpu.make_async_copy(source_ref.at[:, at], own.at[:, at], own_sem.at[i])
        for i, at in enumerate((pl.ds(0, WIDE), pl.ds(WIDE, width - WIDE)))
    ]

    small = [
        pltpu.make_async_copy(low_hbm, low_ref, small_sem.at[0]),
        pltpu.make_async_copy(weight_hbm, weight_ref, small_sem.at[1]),
    ]
    for c in small:
        c.start()
    loads[0].start()

    def by_device(chosen, act, where):
        for i in range(parts):
            mine = [leg for leg in chosen if leg[where] == i]

            if mine:
                @pl.when(me == i)
                def _():
                    for leg in mine:
                        act(leg)

    loads[1].start()

    def send(leg, j):
        s, d, relayed, to_relay, at, to, n, half = leg
        cuts = [n * i // PIECES for i in range(PIECES + 1)]
        for low, high in zip(cuts, cuts[1:]):
            if high > low:
                copy((s, d, relayed, to_relay, at + low, to + low, high - low, half), j).start()

    def copy(leg, j):
        _, target, relayed, to_relay, at, to, n, half = leg
        src, dst = (held if relayed else sent), (held if to_relay else recv)
        return pltpu.make_async_remote_copy(
            src_ref=src.at[j, pl.ds(at, n)],
            dst_ref=dst.at[j, pl.ds(to, n)],
            send_sem=send_sem.at[int(relayed)],
            recv_sem=held_sem.at[half, j] if to_relay else recv_sem.at[j],
            device_id={"rows": target},
            device_id_type=MESH,
        )

    def leave(chosen, j):
        by_device(chosen, lambda leg: send(leg, j), 0)

    def hint_copy(flow):
        k = hop_list.index(flow[1] - flow[0])
        return pltpu.make_async_remote_copy(
            src_ref=early.at[k],
            dst_ref=hint.at[k],
            send_sem=early_send.at[k],
            recv_sem=early_recv.at[k],
            device_id={"rows": flow[1]},
            device_id_type=MESH,
        )

    first_hop = [leg for leg in groups if not leg[2]]
    at_relay = [
        (a, b)
        for a in groups
        for b in groups
        if a[3] and b[2] and a[1] == b[0] and a[5] == b[4] and a[6] == b[6]
    ]

    for c in small:
        c.wait()
    out_w[...] = send_weights(total, parts, me, block, send_rows, low_ref, weight_ref)
    sent_rows = sent.reshape(chunks, send_rows * SUB, LANES)

    def prepare(j):
        y = dot(out_w[...], triple(own[:, columns(j, WIDE)]))
        for b in range(SUB):
            sent_rows[j, pl.ds(b, send_rows, stride=SUB), :] = y[:, b * LANES : (b + 1) * LANES]

    loads[0].wait()
    prepare(0)
    pl.semaphore_wait(barrier, table(me, [len(m) + owners - 1 for m in met]))
    if stepped:
        greet(met_sem)
    here = [leg for leg in first_hop if not stepped or near(*leg[:2])]
    leave(here, 0)

    coarse_w[...] = coarse_weights(total, parts, me, block, low_ref, weight_ref)
    last, known = chunks - 1, chunks - HINTED
    eighth = block >> 3
    loads[1].wait()
    for h in range(HINTED):
        y = pool_columns(dot(coarse_w[...], triple(own[:, columns(known + h, WIDE)])), 3)
        for k in range(len(hop_list)):
            early[k, :, columns(h, WIDE >> 3)] = y[(k + 1) * eighth : (k + 2) * eighth]
        for i in range(owners):
            three[i, :, columns(known + h, WIDE >> 3)] = y[i * each : (i + 1) * each]
    if stepped:
        pl.semaphore_wait(met_sem, table(me, [len(m) for m in met]))
        leave([leg for leg in first_hop if leg not in here], 0)
    by_device(sorted(flows(total, parts)), lambda flow: hint_copy(flow).start(), 0)

    @pl.loop(1, chunks)
    def _(j):
        prepare(j)
        leave(first_hop, j)

    in_w[...] = own_weights(total, parts, me, block, slots, low_ref, weight_ref)

    def forward(j, soon):
        def act(pair):
            copy(pair[0], j).wait_recv()
            send(pair[1], j)

        for i in range(parts):
            mine = [
                (a, b) for a, b in at_relay if b[0] == i and (a[0] // 2 == b[1] // 2) == soon
            ]

            if mine:
                @pl.when(me == i)
                def _():
                    for pair in mine:
                        act(pair)

    def whole(ref, sem):
        return pltpu.make_async_remote_copy(
            src_ref=ref,
            dst_ref=ref,
            send_sem=sem,
            recv_sem=sem,
            device_id={"cols": lax.rem(col + 1, owners)},
            device_id_type=MESH,
        )

    def arrive(j):
        for i in range(parts):
            if rows_in[i]:
                @pl.when(me == i)
                def _():
                    whole(recv.at[j, pl.ds(0, rows_in[i])], recv_sem.at[j]).wait_recv()

    @pl.loop(0, chunks)
    def _(j):
        forward(j, True)

    forward(0, False)

    def compute(x, j):
        rows = chunk_rows(block, in_w, x, (0, 1, 2))
        merc_ref[:, columns(j, WIDE)] = rows[0]
        for level, ref in ((1, one_ref), (2, two_ref)):
            ref[:, columns(j, WIDE >> level)] = pool_columns(rows[level], level)

    def coarse(x, j):
        pooled = pool_columns(chunk_rows(block, in_w, x, (3,))[0], 3)
        for i in range(owners):
            three[i, :, columns(j, WIDE >> 3)] = pooled[i * each : (i + 1) * each]

    def receive(j):
        forward(j + 1, False)
        arrive(j)
        return chunk_operand(total, parts, j, own, recv)

    @pl.loop(0, known - 1)
    def _(j):
        x = receive(j)
        compute(x, j)
        coarse(x, j)

    by_device(sorted(flows(total, parts)), lambda flow: hint_copy(flow).wait_recv(), 1)
    for k, hop in enumerate(hop_list):
        there = table(me, [int((i - hop, i) in flows(total, parts)) for i in range(parts)]) > 0
        part = jnp.where(there, hint[k], 0.0)
        for i in range(owners):
            three[i, :, pl.ds(known * (WIDE >> 3), HINTED * (WIDE >> 3))] += part[i * each : (i + 1) * each]

    x = receive(known - 1)
    coarse(x, known - 1)
    for i in range(1, owners):
        target = lax.rem(col + i, owners)
        pltpu.make_async_remote_copy(
            src_ref=three.at[target],
            dst_ref=landed.at[owners - i],
            send_sem=share_sem.at[0],
            recv_sem=share_sem.at[1],
            device_id={"cols": target},
            device_id_type=MESH,
        ).start()
    compute(x, known - 1)

    @pl.loop(known, last)
    def _(j):
        compute(receive(j), j)

    landed[0] = three[col]
    others = landed.at[pl.ds(1, owners - 1)]
    whole(others, share_sem.at[1]).wait_recv()
    finish(owners, col, landed, rows_ref, pooled_ref)
    whole(others, share_sem.at[0]).wait_send()
    by_device(sorted(flows(total, parts)), lambda flow: hint_copy(flow).wait_send(), 0)
    arrive(last)
    for i in range(parts):
        held_rows = sum(leg[6] for leg in groups if leg[2] and leg[0] == i)

        @pl.when(me == i)
        def _():
            if rows_out[i]:
                whole(sent.at[:, pl.ds(0, rows_out[i])], send_sem.at[0]).wait_send()
            if held_rows:
                whole(held.at[:, pl.ds(0, held_rows)], send_sem.at[1]).wait_send()


def finish(owners, col, landed, rows_ref, pooled_ref):
    _, each, width = landed.shape
    pairs = each // 2
    slab = 2 * LANES
    pairing = jnp.where(
        iota((slab, LANES), 0) >> 1 == iota((slab, LANES), 1), 0.25, 0.0
    ).astype(jnp.bfloat16)
    x = jnp.concatenate([landed[lax.rem(c - col + owners, owners)] for c in range(owners)], axis=1)
    rows_ref[...] = x
    sums = jnp.concatenate(
        [x[2 * p : 2 * p + 1] + x[2 * p + 1 : 2 * p + 2] for p in range(pairs)], axis=0
    )
    count = owners * width // slab
    flat = jnp.concatenate([sums[:, k * slab : (k + 1) * slab] for k in range(count)], axis=0)
    high, low_part = split(flat)
    out = jnp.dot(high, pairing, preferred_element_type=jnp.float32)
    out = out + jnp.dot(low_part, pairing, preferred_element_type=jnp.float32)
    pooled_ref[...] = jnp.concatenate(
        [out[k * pairs : (k + 1) * pairs] for k in range(count)], axis=1
    )


def write_kernel(
    total, parts,
    merc_ref, one_ref, two_ref, rows_ref, pooled_ref, own, recv, in_w,
    merc_out, one_out, two_out, rows_out, pooled_out,
    merc_last, one_last, two_last, sems,
):
    last = own.shape[1] // WIDE - 1
    copies = []

    def put(src, dst):
        copies.append(pltpu.make_async_copy(src, dst, sems.at[len(copies)]))
        copies[-1].start()

    levels = ((merc_ref, merc_out, merc_last), (one_ref, one_out, one_last), (two_ref, two_out, two_last))
    for level, (ref, out, _) in enumerate(levels):
        early = pl.ds(0, last * (WIDE >> level))
        put(ref.at[:, early], out.at[:, early])
    put(rows_ref, rows_out)
    put(pooled_ref, pooled_out)
    x = chunk_operand(total, parts, last, own, recv)
    rows = chunk_rows(own.shape[0], in_w, x, (0, 1, 2))
    for level, (_, out, ref) in enumerate(levels):
        ref[...] = pool_columns(rows[level], level) if level else rows[0]
        put(ref, out.at[:, pl.ds(last * (WIDE >> level), WIDE >> level)])
    for c in copies:
        c.wait()


def body(parts, owners, source, low_row, weight_low):
    total = low_row.shape[0]
    block, width = source.shape
    _, _, sent, got = offsets(total, parts)
    send_rows, slots = up(max(sent), 16), up(max(got), 16)
    hold = max([n for by in relays(total, parts).values() for n in by.values()], default=1)
    hops_out = len(all_hops(total, parts))
    chunks = width // WIDE
    each = (block >> 3) // owners
    wide_rows = block + block // 2 + block // 4 + block // 8
    f32, bf16 = jnp.float32, jnp.bfloat16
    shapes = [(block >> k, width >> k) for k in range(3)]
    shapes += [(each, owners * (width >> 3)), (each // 2, owners * (width >> 4))]
    kept = [pltpu.VMEM(s, f32) for s in shapes]
    kept += [
        pltpu.VMEM((block, width), f32),
        pltpu.VMEM((chunks, slots, SUB, LANES), f32),
        pltpu.VMEM((wide_rows, 3 * (block + slots)), bf16),
    ]
    vmem = pl.BlockSpec(memory_space=pltpu.VMEM)
    hbm = pl.BlockSpec(memory_space=pltpu.HBM)
    dma = pltpu.SemaphoreType.DMA
    outs = pl.pallas_call(
        functools.partial(fused_kernel, total, parts, owners),
        out_shape=kept,
        in_specs=[hbm] * 3,
        out_specs=[vmem] * len(kept),
        scratch_shapes=[
            pltpu.VMEM((parts, block), jnp.int32),
            pltpu.VMEM((parts, block), f32),
            pltpu.VMEM((chunks, send_rows, SUB, LANES), f32),
            pltpu.VMEM((chunks, hold, SUB, LANES), f32),
            pltpu.VMEM((owners, each, width >> 3), f32),
            pltpu.VMEM((owners, each, width >> 3), f32),
            pltpu.VMEM((send_rows, 3 * block), bf16),
            pltpu.VMEM(((1 + hops_out) * (block >> 3), 3 * block), bf16),
            pltpu.VMEM((hops_out, block >> 3, HINTED * (WIDE >> 3)), f32),
            pltpu.VMEM((hops_out, block >> 3, HINTED * (WIDE >> 3)), f32),
            dma((2,)),
            dma((2,)),
            dma((2,)),
            dma((chunks,)),
            dma((2, chunks)),
            dma((hops_out,)),
            dma((hops_out,)),
            dma((2,)),
            pltpu.SemaphoreType.REGULAR,
        ],
        compiler_params=pltpu.CompilerParams(
            collective_id=0, has_side_effects=True, vmem_limit_bytes=47 << 20
        ),
        name="reproject",
    )(low_row.reshape(parts, block), weight_low.reshape(parts, block), source)
    return pl.pallas_call(
        functools.partial(write_kernel, total, parts),
        out_shape=[jax.ShapeDtypeStruct(s, f32) for s in shapes],
        in_specs=[vmem] * len(kept),
        out_specs=[hbm] * len(shapes),
        scratch_shapes=[pltpu.VMEM((block >> k, WIDE >> k), f32) for k in range(3)]
        + [dma((len(shapes) + 3,))],
        compiler_params=pltpu.CompilerParams(vmem_limit_bytes=24 << 20),
        name="write",
    )(*outs)


def solution(mesh):
    return jax.shard_map(
        functools.partial(body, mesh.shape["rows"], mesh.shape["cols"]),
        mesh=mesh,
        in_specs=(P("rows", "cols"), P(), P()),
        out_specs=(
            P("rows", "cols"),
            P("rows", "cols"),
            P("rows", "cols"),
            P(("rows", "cols"), None),
            P(("rows", "cols"), None),
        ),
        check_vma=False,
    )
```

```python
import functools
import math

import jax
import jax.numpy as jnp
import numpy as np
from jax import lax
from jax.experimental import pallas as pl
from jax.experimental.pallas import tpu as pltpu
from jax.sharding import PartitionSpec as P

LANES = 128
SUB = 8
WIDE = SUB * LANES
JITTER = 2
HINTED = 2
MESH = pl.DeviceIdType.MESH


def table(index, values):
    out = jnp.int32(values[0])
    for i in range(1, len(values)):
        if values[i] != values[i - 1]:
            out = jnp.where(index >= i, jnp.int32(values[i]), out)
    return out


@functools.lru_cache(maxsize=None)
def windows(total):
    top = 68.0 * math.pi / 180.0
    edge = math.log(math.tan(math.pi / 4 + top / 2))
    m = np.arange(total, dtype=np.float64)
    y = edge * (1.0 - (2.0 * m + 1.0) / (2.0 * total))
    lat = 2.0 * np.arctan(np.exp(y)) - math.pi / 2
    pos = (top - lat) / top * total - 0.5
    slack = 0.01 * total / 1024
    first = np.clip(np.clip(np.floor(pos - slack), 0, total - 2) - JITTER, 0, total - 2)
    last = np.clip(np.clip(np.floor(pos + slack), 0, total - 2) + JITTER, 0, total - 2) + 1
    return first.astype(int), last.astype(int)


@functools.lru_cache(maxsize=None)
def flows(total, parts):
    first, last = windows(total)
    block = total // parts
    found = {}
    for d in range(parts):
        mine = np.arange(d * block, (d + 1) * block)
        for s in range(parts):
            low, high = s * block, (s + 1) * block
            ms = mine[(last[mine] >= low) & (first[mine] < high)]
            if s == d or not len(ms):
                continue
            a, b = max(low, int(first[ms].min())), min(high - 1, int(last[ms].max()))
            m0, n = int(ms.min()), int(ms.max() - ms.min()) + 1
            found[s, d] = (False, a, b - a + 1) if b - a + 1 <= n else (True, m0, n)
    return found


def offsets(total, parts):
    send, recv, sent, got = {}, {}, [0] * parts, [0] * parts
    for (s, d), (_, _, n) in sorted(flows(total, parts).items()):
        send[s, d], recv[s, d] = sent[s], got[d]
        sent[s] += n
        got[d] += n
    return send, recv, sent, got


@functools.lru_cache(maxsize=None)
def relays(total, parts):
    moves = {k: n for k, (_, _, n) in flows(total, parts).items()}
    pairs = parts // 2
    if parts % 2 or min((d - s for s, d in moves), default=1) < 1 or max((d - s for s, d in moves), default=0) > 2:
        return {}
    plan, taken = {}, set()
    load = [moves.get((2 * z, 2 * z + 1), 0) for z in range(pairs)]
    across = 0.0
    mean = sum(load) / pairs
    for z in range(pairs - 1):
        across += load[z] - mean
        n = int(round(abs(across)))
        at = z if across > 0 else z + 1
        key, relay = (2 * at, 2 * at + 1), 2 * at + (3 if across > 0 else -1)
        if n and n < moves.get(key, 0) and relay not in taken:
            plan.setdefault(key, {})[relay] = n
            taken.add(relay)
    back = [moves.get((2 * z + 1, 2 * z + 2), 0) for z in range(pairs - 1)]
    goal = sum(back) / pairs
    over = 0
    for z in range(pairs - 1):
        want = int(round(goal * (0.975 if z == 0 else 1.0))) - over
        n = max(0, min(want, back[z]))
        if n and 2 * z not in taken:
            plan.setdefault((2 * z + 1, 2 * z + 2), {})[2 * z] = n
            taken.add(2 * z)
            over = back[z] - n
        else:
            over = back[z]
    return plan


def near(i, j):
    return i // 2 == j // 2 or abs(i - j) == 2


def halves(n):
    return [(0, n // 2), (n // 2, n - n // 2)] if n > 1 else [(0, n)]


@functools.lru_cache(maxsize=None)
def legs(total, parts):
    send, recv, _, _ = offsets(total, parts)
    found = []
    for (s, d), (_, _, n) in sorted(flows(total, parts).items()):
        at = 0
        for relay, rows in sorted(relays(total, parts).get((s, d), {}).items()):
            for half, (low, n_part) in enumerate(halves(rows)):
                found.append((s, relay, False, True, send[s, d] + at + low, low, n_part, half))
                found.append((relay, d, True, False, low, recv[s, d] + at + low, n_part, half))
            at += rows
        if n > at:
            found.append((s, d, False, False, send[s, d] + at, recv[s, d] + at, n - at, 0))
    return sorted(found, key=lambda leg: not leg[3])


def up(n, k):
    return -(-n // k) * k


def split(x):
    high = x.astype(jnp.bfloat16)
    low = (x - high.astype(jnp.float32)).astype(jnp.bfloat16)
    return high, low


def iota(shape, axis):
    return lax.broadcasted_iota(jnp.int32, shape, axis)


def pool_columns(x, levels):
    rows, width = x.shape
    slab = LANES << levels
    pairing = jnp.where(
        iota((slab, LANES), 0) >> levels == iota((slab, LANES), 1), 0.5**levels, 0.0
    ).astype(jnp.bfloat16)
    pieces = width // slab
    stacked = jnp.concatenate([x[:, k * slab : (k + 1) * slab] for k in range(pieces)], axis=0)
    high, low = split(stacked)
    out = jnp.dot(high, pairing, preferred_element_type=jnp.float32)
    out = out + jnp.dot(low, pairing, preferred_element_type=jnp.float32)
    return jnp.concatenate([out[k * rows : (k + 1) * rows] for k in range(pieces)], axis=1)


def exact_dot(a, b):
    return lax.dot_general(
        a,
        b,
        (((1,), (1,)), ((), ())),
        precision=lax.Precision.HIGHEST,
        preferred_element_type=jnp.float32,
    )


def flow_tables(total, parts, me, delta, kind, sending):
    send, recv, _, _ = offsets(total, parts)
    rows, place, first = [], [], []
    for i in range(parts):
        key = (i, i + delta) if sending else (i - delta, i)
        what = flows(total, parts).get(key)
        good = what is not None and what[0] == kind
        rows.append(what[2] if good else 0)
        place.append((send if sending else recv)[key] if good else 0)
        first.append(what[1] if good else 0)
    return table(me, rows), table(me, place), table(me, first)


def hops(total, parts, kind):
    return sorted({d - s for (s, d), what in flows(total, parts).items() if what[0] == kind})


def send_weights(total, parts, me, block, rows, low_ref, weight_ref):
    k, c = iota((rows, block), 0), iota((rows, block), 1)
    high = jnp.zeros((rows, block), jnp.float32)
    low_part = high
    for delta in hops(total, parts, False):
        n, at, first = flow_tables(total, parts, me, delta, False, True)
        here = (k >= at) & (k < at + n)
        high = high + jnp.where(here & (c == k - at + first - me * block), 1.0, 0.0)
    for delta in hops(total, parts, True):
        n, at, first = flow_tables(total, parts, me, delta, True, True)
        owner = jnp.clip(me + delta, 0, parts - 1)
        low = low_ref[pl.ds(owner, 1), :] - me * block
        weight = weight_ref[pl.ds(owner, 1), :]
        row = iota((block, block), 0)
        band = jnp.where(row == low, weight, 0.0) + jnp.where(row == low + 1, 1.0 - weight, 0.0)
        pick = (k >= at) & (k < at + n) & (c == k - at + first - owner * block)
        both = lax.dot_general(
            jnp.where(pick, 1.0, 0.0).astype(jnp.bfloat16),
            jnp.concatenate(split(band), axis=0),
            (((1,), (1,)), ((), ())),
            preferred_element_type=jnp.float32,
        )
        high, low_part = high + both[:, :block], low_part + both[:, block:]
    high, low_part = high.astype(jnp.bfloat16), low_part.astype(jnp.bfloat16)
    return jnp.concatenate([high, high, low_part], axis=1)


def pool_rows(block, level):
    o, i = iota((block >> level, block), 0), iota((block >> level, block), 1)
    return jnp.where(i >> level == o, 0.5**level, 0.0).astype(jnp.float32)


def all_hops(total, parts):
    return sorted({d - s for s, d in flows(total, parts)})


def coarse_weights(total, parts, me, block, low_ref, weight_ref):
    out = []
    row = iota((block, block), 0)
    for delta in [0] + all_hops(total, parts):
        owner = jnp.clip(me + delta, 0, parts - 1)
        low = low_ref[pl.ds(owner, 1), :] - me * block
        weight = weight_ref[pl.ds(owner, 1), :]
        band = jnp.where(row == low, weight, 0.0) + jnp.where(row == low + 1, 1.0 - weight, 0.0)
        out.append(exact_dot(pool_rows(block, 3), band))
    high, low_part = split(jnp.concatenate(out, axis=0))
    return jnp.concatenate([high, high, low_part], axis=1)


def own_weights(total, parts, me, block, slots, low_ref, weight_ref):
    low = low_ref[pl.ds(me, 1), :]
    weight = weight_ref[pl.ds(me, 1), :]

    def rows_of(g, valid):
        out = jnp.where(valid & (g == low), weight, 0.0)
        return out + jnp.where(valid & (g == low + 1), 1.0 - weight, 0.0)

    own = iota((block, block), 0) + me * block
    k, m = iota((slots, block), 0), iota((slots, block), 1)
    far = jnp.zeros((slots, block), jnp.float32)
    for delta in hops(total, parts, False):
        n, at, first = flow_tables(total, parts, me, delta, False, False)
        far = far + rows_of(k - at + first, (k >= at) & (k < at + n))
    for delta in hops(total, parts, True):
        n, at, first = flow_tables(total, parts, me, delta, True, False)
        here = (k >= at) & (k < at + n) & (m == k - at + first - me * block)
        far = far + jnp.where(here, 1.0, 0.0)
    band = jnp.concatenate([rows_of(own, own >= 0), far], axis=0)
    pools = [pool_rows(block, level) for level in range(4)]
    high, low_part = split(exact_dot(jnp.concatenate(pools, axis=0), band))
    return jnp.concatenate([high, high, low_part], axis=1)


def columns(j, size):
    return pl.ds(pl.multiple_of(j * size, size), size)


def triple(x):
    high, low_part = split(x)
    return jnp.concatenate([high, low_part, high], axis=0)


def dot(a, b):
    return jnp.dot(a, b, preferred_element_type=jnp.float32)


def chunk_operand(total, parts, j, own, recv):
    chunks, slots = recv.shape[:2]
    got = table(lax.axis_index("rows"), offsets(total, parts)[3])
    rows = recv.reshape(chunks, slots * SUB, LANES)
    row = iota((slots, LANES), 0)
    far = [
        jnp.where(row < got, rows[j, pl.ds(b, slots, stride=SUB), :], 0.0) for b in range(SUB)
    ]
    return triple(
        jnp.concatenate([own[:, columns(j, WIDE)], jnp.concatenate(far, axis=1)], axis=0)
    )


def chunk_rows(block, in_w, x, levels):
    at = [2 * block - (2 * block >> level) for level in levels]
    y = dot(in_w[at[0] : at[-1] + (block >> levels[-1]), :], x)
    return [y[a - at[0] : a - at[0] + (block >> level)] for a, level in zip(at, levels)]


def fused_kernel(
    total, parts, owners,
    low_hbm, weight_hbm, source_ref,
    merc_ref, one_ref, two_ref, rows_ref, pooled_ref, own, recv, in_w,
    low_ref, weight_ref, sent, held, three, landed, out_w, coarse_w, early, hint,
    small_sem, own_sem, send_sem, recv_sem, held_sem, early_send, early_recv, share_sem, met_sem,
):
    block, width = source_ref.shape
    chunks = width // WIDE
    me, col = lax.axis_index("rows"), lax.axis_index("cols")
    groups = legs(total, parts)
    _, _, rows_out, rows_in = offsets(total, parts)
    slots = recv.shape[1]
    send_rows = sent.shape[1]
    each = three.shape[1]
    hop_list = all_hops(total, parts)

    barrier = pltpu.get_barrier_semaphore()
    ties = {leg[:2] for leg in groups} | set(flows(total, parts))
    met = [[j for j in range(parts) if (i, j) in ties or (j, i) in ties] for i in range(parts)]
    stepped = bool(relays(total, parts))
    if stepped:
        met = [[j for j in range(parts) if j != i and near(i, j)] for i in range(parts)]

    def greet(sem):
        for i in range(parts):
            @pl.when(me == i)
            def _():
                for j in met[i]:
                    pl.semaphore_signal(sem, inc=1, device_id={"rows": j}, device_id_type=MESH)

    greet(barrier)
    for i in range(1, owners):
        pl.semaphore_signal(
            barrier, inc=1, device_id={"cols": lax.rem(col + i, owners)}, device_id_type=MESH
        )

    loads = [
        pltpu.make_async_copy(source_ref.at[:, at], own.at[:, at], own_sem.at[i])
        for i, at in enumerate((pl.ds(0, WIDE), pl.ds(WIDE, width - WIDE)))
    ]

    small = [
        pltpu.make_async_copy(low_hbm, low_ref, small_sem.at[0]),
        pltpu.make_async_copy(weight_hbm, weight_ref, small_sem.at[1]),
    ]
    for c in small:
        c.start()
    loads[0].start()

    def by_device(chosen, act, where):
        for i in range(parts):
            mine = [leg for leg in chosen if leg[where] == i]

            if mine:
                @pl.when(me == i)
                def _():
                    for leg in mine:
                        act(leg)

    loads[1].start()

    def copy(leg, j):
        _, target, relayed, to_relay, at, to, n, half = leg
        src, dst = (held if relayed else sent), (held if to_relay else recv)
        return pltpu.make_async_remote_copy(
            src_ref=src.at[j, pl.ds(at, n)],
            dst_ref=dst.at[j, pl.ds(to, n)],
            send_sem=send_sem.at[int(relayed)],
            recv_sem=held_sem.at[half, j] if to_relay else recv_sem.at[j],
            device_id={"rows": target},
            device_id_type=MESH,
        )

    def leave(chosen, j):
        by_device(chosen, lambda leg: copy(leg, j).start(), 0)

    def hint_copy(flow):
        k = hop_list.index(flow[1] - flow[0])
        return pltpu.make_async_remote_copy(
            src_ref=early.at[k],
            dst_ref=hint.at[k],
            send_sem=early_send.at[k],
            recv_sem=early_recv.at[k],
            device_id={"rows": flow[1]},
            device_id_type=MESH,
        )

    first_hop = [leg for leg in groups if not leg[2]]
    at_relay = [
        (a, b)
        for a in groups
        for b in groups
        if a[3] and b[2] and a[1] == b[0] and a[5] == b[4] and a[6] == b[6]
    ]

    for c in small:
        c.wait()
    out_w[...] = send_weights(total, parts, me, block, send_rows, low_ref, weight_ref)
    sent_rows = sent.reshape(chunks, send_rows * SUB, LANES)

    def prepare(j):
        y = dot(out_w[...], triple(own[:, columns(j, WIDE)]))
        for b in range(SUB):
            sent_rows[j, pl.ds(b, send_rows, stride=SUB), :] = y[:, b * LANES : (b + 1) * LANES]

    loads[0].wait()
    prepare(0)
    pl.semaphore_wait(barrier, table(me, [len(m) + owners - 1 for m in met]))
    here = [leg for leg in first_hop if not stepped or near(*leg[:2])]
    leave(here, 0)
    if stepped:
        greet(met_sem)

    coarse_w[...] = coarse_weights(total, parts, me, block, low_ref, weight_ref)
    last, known = chunks - 1, chunks - HINTED
    eighth = block >> 3
    loads[1].wait()
    for h in range(HINTED):
        y = pool_columns(dot(coarse_w[...], triple(own[:, columns(known + h, WIDE)])), 3)
        for k in range(len(hop_list)):
            early[k, :, columns(h, WIDE >> 3)] = y[(k + 1) * eighth : (k + 2) * eighth]
        for i in range(owners):
            three[i, :, columns(known + h, WIDE >> 3)] = y[i * each : (i + 1) * each]
    if stepped:
        pl.semaphore_wait(met_sem, table(me, [len(m) for m in met]))
        leave([leg for leg in first_hop if leg not in here], 0)
    by_device(sorted(flows(total, parts)), lambda flow: hint_copy(flow).start(), 0)

    @pl.loop(1, chunks)
    def _(j):
        prepare(j)
        leave(first_hop, j)

    in_w[...] = own_weights(total, parts, me, block, slots, low_ref, weight_ref)

    def forward(j, soon):
        def act(pair):
            copy(pair[0], j).wait_recv()
            copy(pair[1], j).start()

        for i in range(parts):
            mine = [
                (a, b) for a, b in at_relay if b[0] == i and (a[0] // 2 == b[1] // 2) == soon
            ]

            if mine:
                @pl.when(me == i)
                def _():
                    for pair in mine:
                        act(pair)

    def whole(ref, sem):
        return pltpu.make_async_remote_copy(
            src_ref=ref,
            dst_ref=ref,
            send_sem=sem,
            recv_sem=sem,
            device_id={"cols": lax.rem(col + 1, owners)},
            device_id_type=MESH,
        )

    def arrive(j):
        for i in range(parts):
            if rows_in[i]:
                @pl.when(me == i)
                def _():
                    whole(recv.at[j, pl.ds(0, rows_in[i])], recv_sem.at[j]).wait_recv()

    @pl.loop(0, chunks)
    def _(j):
        forward(j, True)

    forward(0, False)

    def compute(x, j):
        rows = chunk_rows(block, in_w, x, (0, 1, 2))
        merc_ref[:, columns(j, WIDE)] = rows[0]
        for level, ref in ((1, one_ref), (2, two_ref)):
            ref[:, columns(j, WIDE >> level)] = pool_columns(rows[level], level)

    def coarse(x, j):
        pooled = pool_columns(chunk_rows(block, in_w, x, (3,))[0], 3)
        for i in range(owners):
            three[i, :, columns(j, WIDE >> 3)] = pooled[i * each : (i + 1) * each]

    def receive(j):
        forward(j + 1, False)
        arrive(j)
        return chunk_operand(total, parts, j, own, recv)

    @pl.loop(0, known - 1)
    def _(j):
        x = receive(j)
        compute(x, j)
        coarse(x, j)

    by_device(sorted(flows(total, parts)), lambda flow: hint_copy(flow).wait_recv(), 1)
    for k, hop in enumerate(hop_list):
        there = table(me, [int((i - hop, i) in flows(total, parts)) for i in range(parts)]) > 0
        part = jnp.where(there, hint[k], 0.0)
        for i in range(owners):
            three[i, :, pl.ds(known * (WIDE >> 3), HINTED * (WIDE >> 3))] += part[i * each : (i + 1) * each]

    x = receive(known - 1)
    coarse(x, known - 1)
    for i in range(1, owners):
        target = lax.rem(col + i, owners)
        pltpu.make_async_remote_copy(
            src_ref=three.at[target],
            dst_ref=landed.at[owners - i],
            send_sem=share_sem.at[0],
            recv_sem=share_sem.at[1],
            device_id={"cols": target},
            device_id_type=MESH,
        ).start()
    compute(x, known - 1)

    @pl.loop(known, last)
    def _(j):
        compute(receive(j), j)

    landed[0] = three[col]
    others = landed.at[pl.ds(1, owners - 1)]
    whole(others, share_sem.at[1]).wait_recv()
    finish(owners, col, landed, rows_ref, pooled_ref)
    whole(others, share_sem.at[0]).wait_send()
    by_device(sorted(flows(total, parts)), lambda flow: hint_copy(flow).wait_send(), 0)
    arrive(last)
    for i in range(parts):
        held_rows = sum(leg[6] for leg in groups if leg[2] and leg[0] == i)

        @pl.when(me == i)
        def _():
            if rows_out[i]:
                whole(sent.at[:, pl.ds(0, rows_out[i])], send_sem.at[0]).wait_send()
            if held_rows:
                whole(held.at[:, pl.ds(0, held_rows)], send_sem.at[1]).wait_send()


def finish(owners, col, landed, rows_ref, pooled_ref):
    _, each, width = landed.shape
    pairs = each // 2
    slab = 2 * LANES
    pairing = jnp.where(
        iota((slab, LANES), 0) >> 1 == iota((slab, LANES), 1), 0.25, 0.0
    ).astype(jnp.bfloat16)
    x = jnp.concatenate([landed[lax.rem(c - col + owners, owners)] for c in range(owners)], axis=1)
    rows_ref[...] = x
    sums = jnp.concatenate(
        [x[2 * p : 2 * p + 1] + x[2 * p + 1 : 2 * p + 2] for p in range(pairs)], axis=0
    )
    count = owners * width // slab
    flat = jnp.concatenate([sums[:, k * slab : (k + 1) * slab] for k in range(count)], axis=0)
    high, low_part = split(flat)
    out = jnp.dot(high, pairing, preferred_element_type=jnp.float32)
    out = out + jnp.dot(low_part, pairing, preferred_element_type=jnp.float32)
    pooled_ref[...] = jnp.concatenate(
        [out[k * pairs : (k + 1) * pairs] for k in range(count)], axis=1
    )


def write_kernel(
    total, parts,
    merc_ref, one_ref, two_ref, rows_ref, pooled_ref, own, recv, in_w,
    merc_out, one_out, two_out, rows_out, pooled_out,
    merc_last, one_last, two_last, sems,
):
    last = own.shape[1] // WIDE - 1
    copies = []

    def put(src, dst):
        copies.append(pltpu.make_async_copy(src, dst, sems.at[len(copies)]))
        copies[-1].start()

    levels = ((merc_ref, merc_out, merc_last), (one_ref, one_out, one_last), (two_ref, two_out, two_last))
    for level, (ref, out, _) in enumerate(levels):
        early = pl.ds(0, last * (WIDE >> level))
        put(ref.at[:, early], out.at[:, early])
    put(rows_ref, rows_out)
    put(pooled_ref, pooled_out)
    x = chunk_operand(total, parts, last, own, recv)
    rows = chunk_rows(own.shape[0], in_w, x, (0, 1, 2))
    for level, (_, out, ref) in enumerate(levels):
        ref[...] = pool_columns(rows[level], level) if level else rows[0]
        put(ref, out.at[:, pl.ds(last * (WIDE >> level), WIDE >> level)])
    for c in copies:
        c.wait()


def body(parts, owners, source, low_row, weight_low):
    total = low_row.shape[0]
    block, width = source.shape
    _, _, sent, got = offsets(total, parts)
    send_rows, slots = up(max(sent), 16), up(max(got), 16)
    hold = max([n for by in relays(total, parts).values() for n in by.values()], default=1)
    hops_out = len(all_hops(total, parts))
    chunks = width // WIDE
    each = (block >> 3) // owners
    wide_rows = block + block // 2 + block // 4 + block // 8
    f32, bf16 = jnp.float32, jnp.bfloat16
    shapes = [(block >> k, width >> k) for k in range(3)]
    shapes += [(each, owners * (width >> 3)), (each // 2, owners * (width >> 4))]
    kept = [pltpu.VMEM(s, f32) for s in shapes]
    kept += [
        pltpu.VMEM((block, width), f32),
        pltpu.VMEM((chunks, slots, SUB, LANES), f32),
        pltpu.VMEM((wide_rows, 3 * (block + slots)), bf16),
    ]
    vmem = pl.BlockSpec(memory_space=pltpu.VMEM)
    hbm = pl.BlockSpec(memory_space=pltpu.HBM)
    dma = pltpu.SemaphoreType.DMA
    outs = pl.pallas_call(
        functools.partial(fused_kernel, total, parts, owners),
        out_shape=kept,
        in_specs=[hbm] * 3,
        out_specs=[vmem] * len(kept),
        scratch_shapes=[
            pltpu.VMEM((parts, block), jnp.int32),
            pltpu.VMEM((parts, block), f32),
            pltpu.VMEM((chunks, send_rows, SUB, LANES), f32),
            pltpu.VMEM((chunks, hold, SUB, LANES), f32),
            pltpu.VMEM((owners, each, width >> 3), f32),
            pltpu.VMEM((owners, each, width >> 3), f32),
            pltpu.VMEM((send_rows, 3 * block), bf16),
            pltpu.VMEM(((1 + hops_out) * (block >> 3), 3 * block), bf16),
            pltpu.VMEM((hops_out, block >> 3, HINTED * (WIDE >> 3)), f32),
            pltpu.VMEM((hops_out, block >> 3, HINTED * (WIDE >> 3)), f32),
            dma((2,)),
            dma((2,)),
            dma((2,)),
            dma((chunks,)),
            dma((2, chunks)),
            dma((hops_out,)),
            dma((hops_out,)),
            dma((2,)),
            pltpu.SemaphoreType.REGULAR,
        ],
        compiler_params=pltpu.CompilerParams(
            collective_id=0, has_side_effects=True, vmem_limit_bytes=47 << 20
        ),
        name="reproject",
    )(low_row.reshape(parts, block), weight_low.reshape(parts, block), source)
    return pl.pallas_call(
        functools.partial(write_kernel, total, parts),
        out_shape=[jax.ShapeDtypeStruct(s, f32) for s in shapes],
        in_specs=[vmem] * len(kept),
        out_specs=[hbm] * len(shapes),
        scratch_shapes=[pltpu.VMEM((block >> k, WIDE >> k), f32) for k in range(3)]
        + [dma((len(shapes) + 3,))],
        compiler_params=pltpu.CompilerParams(vmem_limit_bytes=24 << 20),
        name="write",
    )(*outs)


def solution(mesh):
    return jax.shard_map(
        functools.partial(body, mesh.shape["rows"], mesh.shape["cols"]),
        mesh=mesh,
        in_specs=(P("rows", "cols"), P(), P()),
        out_specs=(
            P("rows", "cols"),
            P("rows", "cols"),
            P("rows", "cols"),
            P(("rows", "cols"), None),
            P(("rows", "cols"), None),
        ),
        check_vma=False,
    )
```

```python
import functools
import math

import jax
import jax.numpy as jnp
import numpy as np
from jax import lax
from jax.experimental import pallas as pl
from jax.experimental.pallas import tpu as pltpu
from jax.sharding import PartitionSpec as P

LANES = 128
SUB = 8
WIDE = SUB * LANES
JITTER = 2
HINTED = 2
MESH = pl.DeviceIdType.MESH


def table(index, values):
    out = jnp.int32(values[0])
    for i in range(1, len(values)):
        if values[i] != values[i - 1]:
            out = jnp.where(index >= i, jnp.int32(values[i]), out)
    return out


@functools.lru_cache(maxsize=None)
def windows(total):
    top = 68.0 * math.pi / 180.0
    edge = math.log(math.tan(math.pi / 4 + top / 2))
    m = np.arange(total, dtype=np.float64)
    y = edge * (1.0 - (2.0 * m + 1.0) / (2.0 * total))
    lat = 2.0 * np.arctan(np.exp(y)) - math.pi / 2
    pos = (top - lat) / top * total - 0.5
    slack = 0.01 * total / 1024
    first = np.clip(np.clip(np.floor(pos - slack), 0, total - 2) - JITTER, 0, total - 2)
    last = np.clip(np.clip(np.floor(pos + slack), 0, total - 2) + JITTER, 0, total - 2) + 1
    return first.astype(int), last.astype(int)


@functools.lru_cache(maxsize=None)
def flows(total, parts):
    first, last = windows(total)
    block = total // parts
    found = {}
    for d in range(parts):
        mine = np.arange(d * block, (d + 1) * block)
        for s in range(parts):
            low, high = s * block, (s + 1) * block
            ms = mine[(last[mine] >= low) & (first[mine] < high)]
            if s == d or not len(ms):
                continue
            a, b = max(low, int(first[ms].min())), min(high - 1, int(last[ms].max()))
            m0, n = int(ms.min()), int(ms.max() - ms.min()) + 1
            found[s, d] = (False, a, b - a + 1) if b - a + 1 <= n else (True, m0, n)
    return found


def offsets(total, parts):
    send, recv, sent, got = {}, {}, [0] * parts, [0] * parts
    for (s, d), (_, _, n) in sorted(flows(total, parts).items()):
        send[s, d], recv[s, d] = sent[s], got[d]
        sent[s] += n
        got[d] += n
    return send, recv, sent, got


@functools.lru_cache(maxsize=None)
def relays(total, parts):
    moves = {k: n for k, (_, _, n) in flows(total, parts).items()}
    pairs = parts // 2
    if parts % 2 or min((d - s for s, d in moves), default=1) < 1 or max((d - s for s, d in moves), default=0) > 2:
        return {}
    plan, taken = {}, set()
    load = [moves.get((2 * z, 2 * z + 1), 0) for z in range(pairs)]
    across = 0.0
    mean = sum(load) / pairs
    for z in range(pairs - 1):
        across += load[z] - mean
        n = int(round(abs(across)))
        at = z if across > 0 else z + 1
        key, relay = (2 * at, 2 * at + 1), 2 * at + (3 if across > 0 else -1)
        if n and n < moves.get(key, 0) and relay not in taken:
            plan.setdefault(key, {})[relay] = n
            taken.add(relay)
    back = [moves.get((2 * z + 1, 2 * z + 2), 0) for z in range(pairs - 1)]
    goal = sum(back) / pairs
    over = 0
    for z in range(pairs - 1):
        want = int(round(goal * (0.975 if z == 0 else 1.0))) - over
        n = max(0, min(want, back[z]))
        if n and 2 * z not in taken:
            plan.setdefault((2 * z + 1, 2 * z + 2), {})[2 * z] = n
            taken.add(2 * z)
            over = back[z] - n
        else:
            over = back[z]
    return plan


def near(i, j):
    return i // 2 == j // 2 or abs(i - j) == 2


def halves(n):
    return [(0, n // 2), (n // 2, n - n // 2)] if n > 1 else [(0, n)]


@functools.lru_cache(maxsize=None)
def legs(total, parts):
    send, recv, _, _ = offsets(total, parts)
    found = []
    for (s, d), (_, _, n) in sorted(flows(total, parts).items()):
        at = 0
        for relay, rows in sorted(relays(total, parts).get((s, d), {}).items()):
            for half, (low, n_part) in enumerate(halves(rows)):
                found.append((s, relay, False, True, send[s, d] + at + low, low, n_part, half))
                found.append((relay, d, True, False, low, recv[s, d] + at + low, n_part, half))
            at += rows
        if n > at:
            found.append((s, d, False, False, send[s, d] + at, recv[s, d] + at, n - at, 0))
    return sorted(found, key=lambda leg: not leg[3])


def up(n, k):
    return -(-n // k) * k


def split(x):
    high = x.astype(jnp.bfloat16)
    low = (x - high.astype(jnp.float32)).astype(jnp.bfloat16)
    return high, low


def iota(shape, axis):
    return lax.broadcasted_iota(jnp.int32, shape, axis)


def pool_columns(x, levels):
    rows, width = x.shape
    slab = LANES << levels
    pairing = jnp.where(
        iota((slab, LANES), 0) >> levels == iota((slab, LANES), 1), 0.5**levels, 0.0
    ).astype(jnp.bfloat16)
    pieces = width // slab
    stacked = jnp.concatenate([x[:, k * slab : (k + 1) * slab] for k in range(pieces)], axis=0)
    high, low = split(stacked)
    out = jnp.dot(high, pairing, preferred_element_type=jnp.float32)
    out = out + jnp.dot(low, pairing, preferred_element_type=jnp.float32)
    return jnp.concatenate([out[k * rows : (k + 1) * rows] for k in range(pieces)], axis=1)


def exact_dot(a, b):
    return lax.dot_general(
        a,
        b,
        (((1,), (1,)), ((), ())),
        precision=lax.Precision.HIGHEST,
        preferred_element_type=jnp.float32,
    )


def flow_tables(total, parts, me, delta, kind, sending):
    send, recv, _, _ = offsets(total, parts)
    rows, place, first = [], [], []
    for i in range(parts):
        key = (i, i + delta) if sending else (i - delta, i)
        what = flows(total, parts).get(key)
        good = what is not None and what[0] == kind
        rows.append(what[2] if good else 0)
        place.append((send if sending else recv)[key] if good else 0)
        first.append(what[1] if good else 0)
    return table(me, rows), table(me, place), table(me, first)


def hops(total, parts, kind):
    return sorted({d - s for (s, d), what in flows(total, parts).items() if what[0] == kind})


def send_weights(total, parts, me, block, rows, low_ref, weight_ref):
    k, c = iota((rows, block), 0), iota((rows, block), 1)
    high = jnp.zeros((rows, block), jnp.float32)
    low_part = high
    for delta in hops(total, parts, False):
        n, at, first = flow_tables(total, parts, me, delta, False, True)
        here = (k >= at) & (k < at + n)
        high = high + jnp.where(here & (c == k - at + first - me * block), 1.0, 0.0)
    for delta in hops(total, parts, True):
        n, at, first = flow_tables(total, parts, me, delta, True, True)
        owner = jnp.clip(me + delta, 0, parts - 1)
        low = low_ref[pl.ds(owner, 1), :] - me * block
        weight = weight_ref[pl.ds(owner, 1), :]
        row = iota((block, block), 0)
        band = jnp.where(row == low, weight, 0.0) + jnp.where(row == low + 1, 1.0 - weight, 0.0)
        pick = (k >= at) & (k < at + n) & (c == k - at + first - owner * block)
        both = lax.dot_general(
            jnp.where(pick, 1.0, 0.0).astype(jnp.bfloat16),
            jnp.concatenate(split(band), axis=0),
            (((1,), (1,)), ((), ())),
            preferred_element_type=jnp.float32,
        )
        high, low_part = high + both[:, :block], low_part + both[:, block:]
    high, low_part = high.astype(jnp.bfloat16), low_part.astype(jnp.bfloat16)
    return jnp.concatenate([high, high, low_part], axis=1)


def pool_rows(block, level):
    o, i = iota((block >> level, block), 0), iota((block >> level, block), 1)
    return jnp.where(i >> level == o, 0.5**level, 0.0).astype(jnp.float32)


def all_hops(total, parts):
    return sorted({d - s for s, d in flows(total, parts)})


def coarse_weights(total, parts, me, block, low_ref, weight_ref):
    out = []
    row = iota((block, block), 0)
    for delta in [0] + all_hops(total, parts):
        owner = jnp.clip(me + delta, 0, parts - 1)
        low = low_ref[pl.ds(owner, 1), :] - me * block
        weight = weight_ref[pl.ds(owner, 1), :]
        band = jnp.where(row == low, weight, 0.0) + jnp.where(row == low + 1, 1.0 - weight, 0.0)
        out.append(exact_dot(pool_rows(block, 3), band))
    high, low_part = split(jnp.concatenate(out, axis=0))
    return jnp.concatenate([high, high, low_part], axis=1)


def own_weights(total, parts, me, block, slots, low_ref, weight_ref):
    low = low_ref[pl.ds(me, 1), :]
    weight = weight_ref[pl.ds(me, 1), :]

    def rows_of(g, valid):
        out = jnp.where(valid & (g == low), weight, 0.0)
        return out + jnp.where(valid & (g == low + 1), 1.0 - weight, 0.0)

    own = iota((block, block), 0) + me * block
    k, m = iota((slots, block), 0), iota((slots, block), 1)
    far = jnp.zeros((slots, block), jnp.float32)
    for delta in hops(total, parts, False):
        n, at, first = flow_tables(total, parts, me, delta, False, False)
        far = far + rows_of(k - at + first, (k >= at) & (k < at + n))
    for delta in hops(total, parts, True):
        n, at, first = flow_tables(total, parts, me, delta, True, False)
        here = (k >= at) & (k < at + n) & (m == k - at + first - me * block)
        far = far + jnp.where(here, 1.0, 0.0)
    band = jnp.concatenate([rows_of(own, own >= 0), far], axis=0)
    pools = [pool_rows(block, level) for level in range(4)]
    high, low_part = split(exact_dot(jnp.concatenate(pools, axis=0), band))
    return jnp.concatenate([high, high, low_part], axis=1)


def columns(j, size):
    return pl.ds(pl.multiple_of(j * size, size), size)


def triple(x):
    high, low_part = split(x)
    return jnp.concatenate([high, low_part, high], axis=0)


def dot(a, b):
    return jnp.dot(a, b, preferred_element_type=jnp.float32)


def chunk_operand(total, parts, j, own, recv):
    chunks, slots = recv.shape[:2]
    got = table(lax.axis_index("rows"), offsets(total, parts)[3])
    rows = recv.reshape(chunks, slots * SUB, LANES)
    row = iota((slots, LANES), 0)
    far = [
        jnp.where(row < got, rows[j, pl.ds(b, slots, stride=SUB), :], 0.0) for b in range(SUB)
    ]
    return triple(
        jnp.concatenate([own[:, columns(j, WIDE)], jnp.concatenate(far, axis=1)], axis=0)
    )


def chunk_rows(block, in_w, x, levels):
    at = [2 * block - (2 * block >> level) for level in levels]
    y = dot(in_w[at[0] : at[-1] + (block >> levels[-1]), :], x)
    return [y[a - at[0] : a - at[0] + (block >> level)] for a, level in zip(at, levels)]


def fused_kernel(
    total, parts, owners,
    low_hbm, weight_hbm, source_ref,
    merc_ref, one_ref, two_ref, rows_ref, pooled_ref, own, recv, in_w,
    low_ref, weight_ref, sent, held, three, landed, out_w, coarse_w, early, hint,
    small_sem, own_sem, send_sem, recv_sem, held_sem, early_sem, share_sem, met_sem,
):
    block, width = source_ref.shape
    chunks = width // WIDE
    me, col = lax.axis_index("rows"), lax.axis_index("cols")
    groups = legs(total, parts)
    _, _, rows_out, rows_in = offsets(total, parts)
    slots = recv.shape[1]
    send_rows = sent.shape[1]
    each = three.shape[1]
    hop_list = all_hops(total, parts)

    barrier = pltpu.get_barrier_semaphore()
    ties = {leg[:2] for leg in groups} | set(flows(total, parts))
    met = [[j for j in range(parts) if (i, j) in ties or (j, i) in ties] for i in range(parts)]
    stepped = bool(relays(total, parts))
    if stepped:
        met = [[j for j in range(parts) if j != i and near(i, j)] for i in range(parts)]

    def greet(sem):
        for i in range(parts):
            @pl.when(me == i)
            def _():
                for j in met[i]:
                    pl.semaphore_signal(sem, inc=1, device_id={"rows": j}, device_id_type=MESH)

    greet(barrier)
    for i in range(1, owners):
        pl.semaphore_signal(
            barrier, inc=1, device_id={"cols": lax.rem(col + i, owners)}, device_id_type=MESH
        )

    loads = [
        pltpu.make_async_copy(source_ref.at[:, at], own.at[:, at], own_sem.at[i])
        for i, at in enumerate((pl.ds(0, WIDE), pl.ds(WIDE, width - WIDE)))
    ]

    small = [
        pltpu.make_async_copy(low_hbm, low_ref, small_sem.at[0]),
        pltpu.make_async_copy(weight_hbm, weight_ref, small_sem.at[1]),
    ]
    for c in small:
        c.start()
    loads[0].start()

    def by_device(chosen, act, where):
        for i in range(parts):
            mine = [leg for leg in chosen if leg[where] == i]

            if mine:
                @pl.when(me == i)
                def _():
                    for leg in mine:
                        act(leg)

    loads[1].start()

    def copy(leg, j):
        _, target, relayed, to_relay, at, to, n, half = leg
        src, dst = (held if relayed else sent), (held if to_relay else recv)
        return pltpu.make_async_remote_copy(
            src_ref=src.at[j, pl.ds(at, n)],
            dst_ref=dst.at[j, pl.ds(to, n)],
            send_sem=send_sem.at[int(relayed)],
            recv_sem=held_sem.at[half, j] if to_relay else recv_sem.at[j],
            device_id={"rows": target},
            device_id_type=MESH,
        )

    def leave(chosen, j):
        by_device(chosen, lambda leg: copy(leg, j).start(), 0)

    def hint_copy(flow):
        k = hop_list.index(flow[1] - flow[0])
        return pltpu.make_async_remote_copy(
            src_ref=early.at[k],
            dst_ref=hint.at[k],
            send_sem=early_sem.at[0],
            recv_sem=early_sem.at[1],
            device_id={"rows": flow[1]},
            device_id_type=MESH,
        )

    first_hop = [leg for leg in groups if not leg[2]]
    at_relay = [
        (a, b)
        for a in groups
        for b in groups
        if a[3] and b[2] and a[1] == b[0] and a[5] == b[4] and a[6] == b[6]
    ]

    for c in small:
        c.wait()
    out_w[...] = send_weights(total, parts, me, block, send_rows, low_ref, weight_ref)
    sent_rows = sent.reshape(chunks, send_rows * SUB, LANES)

    def prepare(j):
        y = dot(out_w[...], triple(own[:, columns(j, WIDE)]))
        for b in range(SUB):
            sent_rows[j, pl.ds(b, send_rows, stride=SUB), :] = y[:, b * LANES : (b + 1) * LANES]

    loads[0].wait()
    prepare(0)
    pl.semaphore_wait(barrier, table(me, [len(m) + owners - 1 for m in met]))
    here = [leg for leg in first_hop if not stepped or near(*leg[:2])]
    leave(here, 0)
    if stepped:
        greet(met_sem)

    coarse_w[...] = coarse_weights(total, parts, me, block, low_ref, weight_ref)
    last, known = chunks - 1, chunks - HINTED
    eighth = block >> 3
    loads[1].wait()
    for h in range(HINTED):
        y = pool_columns(dot(coarse_w[...], triple(own[:, columns(known + h, WIDE)])), 3)
        for k in range(len(hop_list)):
            early[k, :, columns(h, WIDE >> 3)] = y[(k + 1) * eighth : (k + 2) * eighth]
        for i in range(owners):
            three[i, :, columns(known + h, WIDE >> 3)] = y[i * each : (i + 1) * each]
    if stepped:
        pl.semaphore_wait(met_sem, table(me, [len(m) for m in met]))
        leave([leg for leg in first_hop if leg not in here], 0)
    by_device(sorted(flows(total, parts)), lambda flow: hint_copy(flow).start(), 0)

    @pl.loop(1, chunks)
    def _(j):
        prepare(j)
        leave(first_hop, j)

    in_w[...] = own_weights(total, parts, me, block, slots, low_ref, weight_ref)

    def forward(j, soon):
        def act(pair):
            copy(pair[0], j).wait_recv()
            copy(pair[1], j).start()

        for i in range(parts):
            mine = [
                (a, b) for a, b in at_relay if b[0] == i and (a[0] // 2 == b[1] // 2) == soon
            ]

            if mine:
                @pl.when(me == i)
                def _():
                    for pair in mine:
                        act(pair)

    def whole(ref, sem):
        return pltpu.make_async_remote_copy(
            src_ref=ref,
            dst_ref=ref,
            send_sem=sem,
            recv_sem=sem,
            device_id={"cols": lax.rem(col + 1, owners)},
            device_id_type=MESH,
        )

    def arrive(j):
        for i in range(parts):
            if rows_in[i]:
                @pl.when(me == i)
                def _():
                    whole(recv.at[j, pl.ds(0, rows_in[i])], recv_sem.at[j]).wait_recv()

    @pl.loop(0, chunks)
    def _(j):
        forward(j, True)

    forward(0, False)

    def compute(x, j):
        rows = chunk_rows(block, in_w, x, (0, 1, 2))
        merc_ref[:, columns(j, WIDE)] = rows[0]
        for level, ref in ((1, one_ref), (2, two_ref)):
            ref[:, columns(j, WIDE >> level)] = pool_columns(rows[level], level)

    def coarse(x, j):
        pooled = pool_columns(chunk_rows(block, in_w, x, (3,))[0], 3)
        for i in range(owners):
            three[i, :, columns(j, WIDE >> 3)] = pooled[i * each : (i + 1) * each]

    def receive(j):
        forward(j + 1, False)
        arrive(j)
        return chunk_operand(total, parts, j, own, recv)

    @pl.loop(0, known - 1)
    def _(j):
        x = receive(j)
        compute(x, j)
        coarse(x, j)

    for i in range(parts):
        count = sum(d == i for _, d in flows(total, parts))
        if count:
            @pl.when(me == i)
            def _():
                whole(hint.at[pl.ds(0, count)], early_sem.at[1]).wait_recv()

    for k, hop in enumerate(hop_list):
        there = table(me, [int((i - hop, i) in flows(total, parts)) for i in range(parts)]) > 0
        part = jnp.where(there, hint[k], 0.0)
        for i in range(owners):
            three[i, :, pl.ds(known * (WIDE >> 3), HINTED * (WIDE >> 3))] += part[i * each : (i + 1) * each]

    x = receive(known - 1)
    coarse(x, known - 1)
    for i in range(1, owners):
        target = lax.rem(col + i, owners)
        pltpu.make_async_remote_copy(
            src_ref=three.at[target],
            dst_ref=landed.at[owners - i],
            send_sem=share_sem.at[0],
            recv_sem=share_sem.at[1],
            device_id={"cols": target},
            device_id_type=MESH,
        ).start()
    compute(x, known - 1)

    @pl.loop(known, last)
    def _(j):
        compute(receive(j), j)

    landed[0] = three[col]
    others = landed.at[pl.ds(1, owners - 1)]
    whole(others, share_sem.at[1]).wait_recv()
    finish(owners, col, landed, rows_ref, pooled_ref)
    whole(others, share_sem.at[0]).wait_send()
    arrive(last)
    for i in range(parts):
        held_rows = sum(leg[6] for leg in groups if leg[2] and leg[0] == i)
        count = sum(a == i for a, _ in flows(total, parts))

        @pl.when(me == i)
        def _():
            if count:
                whole(early.at[pl.ds(0, count)], early_sem.at[0]).wait_send()
            if rows_out[i]:
                whole(sent.at[:, pl.ds(0, rows_out[i])], send_sem.at[0]).wait_send()
            if held_rows:
                whole(held.at[:, pl.ds(0, held_rows)], send_sem.at[1]).wait_send()


def finish(owners, col, landed, rows_ref, pooled_ref):
    _, each, width = landed.shape
    pairs = each // 2
    slab = 2 * LANES
    pairing = jnp.where(
        iota((slab, LANES), 0) >> 1 == iota((slab, LANES), 1), 0.25, 0.0
    ).astype(jnp.bfloat16)
    x = jnp.concatenate([landed[lax.rem(c - col + owners, owners)] for c in range(owners)], axis=1)
    rows_ref[...] = x
    sums = jnp.concatenate(
        [x[2 * p : 2 * p + 1] + x[2 * p + 1 : 2 * p + 2] for p in range(pairs)], axis=0
    )
    count = owners * width // slab
    flat = jnp.concatenate([sums[:, k * slab : (k + 1) * slab] for k in range(count)], axis=0)
    high, low_part = split(flat)
    out = jnp.dot(high, pairing, preferred_element_type=jnp.float32)
    out = out + jnp.dot(low_part, pairing, preferred_element_type=jnp.float32)
    pooled_ref[...] = jnp.concatenate(
        [out[k * pairs : (k + 1) * pairs] for k in range(count)], axis=1
    )


def write_kernel(
    total, parts,
    merc_ref, one_ref, two_ref, rows_ref, pooled_ref, own, recv, in_w,
    merc_out, one_out, two_out, rows_out, pooled_out,
    merc_last, one_last, two_last, sems,
):
    last = own.shape[1] // WIDE - 1
    copies = []

    def put(src, dst):
        copies.append(pltpu.make_async_copy(src, dst, sems.at[len(copies)]))
        copies[-1].start()

    levels = ((merc_ref, merc_out, merc_last), (one_ref, one_out, one_last), (two_ref, two_out, two_last))
    for level, (ref, out, _) in enumerate(levels):
        early = pl.ds(0, last * (WIDE >> level))
        put(ref.at[:, early], out.at[:, early])
    put(rows_ref, rows_out)
    put(pooled_ref, pooled_out)
    x = chunk_operand(total, parts, last, own, recv)
    rows = chunk_rows(own.shape[0], in_w, x, (0, 1, 2))
    for level, (_, out, ref) in enumerate(levels):
        ref[...] = pool_columns(rows[level], level) if level else rows[0]
        put(ref, out.at[:, pl.ds(last * (WIDE >> level), WIDE >> level)])
    for c in copies:
        c.wait()


def body(parts, owners, source, low_row, weight_low):
    total = low_row.shape[0]
    block, width = source.shape
    _, _, sent, got = offsets(total, parts)
    send_rows, slots = up(max(sent), 16), up(max(got), 16)
    hold = max([n for by in relays(total, parts).values() for n in by.values()], default=1)
    hops_out = len(all_hops(total, parts))
    chunks = width // WIDE
    each = (block >> 3) // owners
    wide_rows = block + block // 2 + block // 4 + block // 8
    f32, bf16 = jnp.float32, jnp.bfloat16
    shapes = [(block >> k, width >> k) for k in range(3)]
    shapes += [(each, owners * (width >> 3)), (each // 2, owners * (width >> 4))]
    kept = [pltpu.VMEM(s, f32) for s in shapes]
    kept += [
        pltpu.VMEM((block, width), f32),
        pltpu.VMEM((chunks, slots, SUB, LANES), f32),
        pltpu.VMEM((wide_rows, 3 * (block + slots)), bf16),
    ]
    vmem = pl.BlockSpec(memory_space=pltpu.VMEM)
    hbm = pl.BlockSpec(memory_space=pltpu.HBM)
    dma = pltpu.SemaphoreType.DMA
    outs = pl.pallas_call(
        functools.partial(fused_kernel, total, parts, owners),
        out_shape=kept,
        in_specs=[hbm] * 3,
        out_specs=[vmem] * len(kept),
        scratch_shapes=[
            pltpu.VMEM((parts, block), jnp.int32),
            pltpu.VMEM((parts, block), f32),
            pltpu.VMEM((chunks, send_rows, SUB, LANES), f32),
            pltpu.VMEM((chunks, hold, SUB, LANES), f32),
            pltpu.VMEM((owners, each, width >> 3), f32),
            pltpu.VMEM((owners, each, width >> 3), f32),
            pltpu.VMEM((send_rows, 3 * block), bf16),
            pltpu.VMEM(((1 + hops_out) * (block >> 3), 3 * block), bf16),
            pltpu.VMEM((hops_out, block >> 3, HINTED * (WIDE >> 3)), f32),
            pltpu.VMEM((hops_out, block >> 3, HINTED * (WIDE >> 3)), f32),
            dma((2,)),
            dma((2,)),
            dma((2,)),
            dma((chunks,)),
            dma((2, chunks)),
            dma((2,)),
            dma((2,)),
            pltpu.SemaphoreType.REGULAR,
        ],
        compiler_params=pltpu.CompilerParams(
            collective_id=0, has_side_effects=True, vmem_limit_bytes=47 << 20
        ),
        name="reproject",
    )(low_row.reshape(parts, block), weight_low.reshape(parts, block), source)
    return pl.pallas_call(
        functools.partial(write_kernel, total, parts),
        out_shape=[jax.ShapeDtypeStruct(s, f32) for s in shapes],
        in_specs=[vmem] * len(kept),
        out_specs=[hbm] * len(shapes),
        scratch_shapes=[pltpu.VMEM((block >> k, WIDE >> k), f32) for k in range(3)]
        + [dma((len(shapes) + 3,))],
        compiler_params=pltpu.CompilerParams(vmem_limit_bytes=24 << 20),
        name="write",
    )(*outs)


def solution(mesh):
    return jax.shard_map(
        functools.partial(body, mesh.shape["rows"], mesh.shape["cols"]),
        mesh=mesh,
        in_specs=(P("rows", "cols"), P(), P()),
        out_specs=(
            P("rows", "cols"),
            P("rows", "cols"),
            P("rows", "cols"),
            P(("rows", "cols"), None),
            P(("rows", "cols"), None),
        ),
        check_vma=False,
    )
```
